128 devices in a mesh: row: 8 (over x, y_lo), col: 16 (over y_hi, z, core).
Axes of the slice: x: 4, y: 4 (y_hi: 2, y_lo: 2; y = y_hi * 2 + y_lo), z: 4, core: 2. Of those that a mesh axis runs over, the one named last changes fastest.
Arguments:
- objects: float32 [4, 4096, 8192], P(None, 'row', 'col'), may hold values from -5 to 5
- illumination: float32 [2, 256, 256], replicated, may hold values from -5 to 5
- propagator_phase: float32 [256, 256], replicated, may hold values from -3.140625 to 3.140625
- intensity: bfloat16 [1536, 256, 256], P(('row', 'col')), may hold values from 0 to 2
- offsets: int32 [1536, 2], P(('row', 'col')), may hold values from -1 to 3, as said below
- counts: int32 [128], P(('row', 'col')), may hold values from 0 to 12, as said below
Outputs:
- gradient: float32 [4, 4096, 8192], P(None, 'row', 'col')
The draws below stay inside these ranges and needn't reach their ends.
Inputs may be any that keep to these rules, and one draw needn't show every extreme that they name: `counts`: for every device, its count plus the count of the device 16 // 2 further along col (cyclically, same row) is at most 12; some device has exactly 12; every device at row index 0 has a live slot. `offsets`: the first slot of every device has column offset 512 // 128 - 1.
All inputs are finite; a program needn't handle non-finite values.
Results may differ from the reference program's by a relative error of at most 0.015.
Values may be sent and summed in bfloat16 or wider, within the bound.
A program may use at most 128 MiB of HBM per device.

```python
import math
import jax
import jax.numpy as jnp
from jax import lax

PROBE = 256
TILE = 512
SLOTS = 12
NR = 4096
NC = 8192
TASKS = 1536
N_ROW = 8
N_COL = 16


def draw_counts(key, part):
    half_cols = N_COL // 2
    pair_count = N_ROW * half_cols
    key_total, key_share, key_pick, key_side = jax.random.split(jax.random.fold_in(key, 11), 4)
    totals = jax.random.randint(key_total, (pair_count,), 3 * SLOTS // 4, SLOTS + 1)
    shares = jax.random.randint(key_share, (pair_count,), 1, totals)
    chosen = jax.random.randint(key_pick, (), half_cols, pair_count)
    flip_side = jax.random.randint(key_side, (), 0, 2)
    pair_ids = jnp.arange(pair_count)
    totals = jnp.where(pair_ids == chosen, SLOTS, totals)
    shares = jnp.where(pair_ids == chosen, SLOTS * flip_side, shares)
    first_half = shares.reshape(N_ROW, half_cols)
    second_half = (totals - shares).reshape(N_ROW, half_cols)
    return jnp.concatenate([first_half, second_half], axis=1).reshape(N_ROW * N_COL).astype(jnp.int32)


def draw_offsets(key, part):
    highest = TILE // (PROBE // 2)
    drawn = jax.random.randint(jax.random.fold_in(key, 23), (TASKS, 2), -1, highest)
    first_slot = jnp.arange(TASKS) % SLOTS == 0
    column = jnp.where(first_slot, highest - 1, drawn[:, 1])
    return jnp.stack([drawn[:, 0], column], axis=1).astype(jnp.int32)


def block_scale(stream_key, shape, cuts, low, high):
    loudness, own = 1.0, jax.random.fold_in(stream_key, 6)
    for position, blocks in cuts:
        draws = jnp.exp(jax.random.uniform(jax.random.fold_in(own, position), (blocks,), jnp.float32, low / len(cuts), high / len(cuts)))
        loudness = loudness * jnp.repeat(draws, shape[position] // blocks).reshape([-1 if axis == position else 1 for axis in range(len(shape))])
    return loudness


def centred(key, dims, width, reach, cuts=(), kind=jnp.bfloat16):
    entries = jax.random.normal(key, dims, jnp.float32) * width
    if len(cuts) > 0:
        entries = block_scale(key, dims, cuts, -0.22, 0.18) * entries
    return jnp.clip(entries, min=-reach, max=reach).astype(kind)


def setup_inputs(seed: int = 0) -> dict:
    arg_keys = jax.random.split(jax.random.key(seed), 7)
    objects = centred(arg_keys[0], (4, NR, NC), 0.7, 5.0, ((1, 8), (2, 16)), jnp.float32)
    illumination = centred(arg_keys[1], (2, PROBE, PROBE), 0.7, 5.0, (), jnp.float32)
    propagator_phase = jnp.clip(jax.random.uniform(arg_keys[2], (PROBE, PROBE), jnp.float32, -3.140625, 3.140625), -3.140625, 3.140625)
    intensity = jnp.clip(2.0 * jax.random.uniform(arg_keys[3], (TASKS, PROBE, PROBE), jnp.float32) ** block_scale(arg_keys[3], (TASKS, PROBE, PROBE), ((0, 128),), -0.2, 0.2), 0.0, 2.0).astype(jnp.bfloat16)
    offsets = draw_offsets(jax.random.fold_in(arg_keys[6], 71), 0)
    counts = draw_counts(jax.random.fold_in(arg_keys[6], 71), 0)
    return dict(objects=objects, illumination=illumination, propagator_phase=propagator_phase, intensity=intensity, offsets=offsets, counts=counts)


def tables(extent):
    number = jnp.arange(extent, dtype=jnp.int32)
    turns = number[:, None] * number[None, :] % extent
    angle = turns.astype(jnp.float32) * (2.0 * math.pi / extent)
    scale = 1.0 / math.sqrt(extent)
    return ((jnp.cos(angle) * scale).astype(jnp.bfloat16), (jnp.sin(angle) * scale).astype(jnp.bfloat16))

def left_product(matrix, field):
    return jnp.einsum('jk,bkl->bjl', matrix.astype(jnp.float32), field.astype(jnp.float32))

def right_product(field, matrix):
    return jnp.einsum('bjk,kl->bjl', field.astype(jnp.float32), matrix.astype(jnp.float32))

def transform(field_real, field_imag, direction, cosine_table, sine_table):
    upper_real = (left_product(cosine_table, field_real) + direction * left_product(sine_table, field_imag)).astype(jnp.bfloat16)
    upper_imag = (left_product(cosine_table, field_imag) - direction * left_product(sine_table, field_real)).astype(jnp.bfloat16)
    out_real = right_product(upper_real, cosine_table) + direction * right_product(upper_imag, sine_table)
    out_imag = right_product(upper_imag, cosine_table) - direction * right_product(upper_real, sine_table)
    return (out_real, out_imag)

def complex_product(left_real, left_imag, right_real, right_imag):
    return (left_real * right_real - left_imag * right_imag, left_real * right_imag + left_imag * right_real)

def to_half(pair):
    return (pair[0].astype(jnp.bfloat16), pair[1].astype(jnp.bfloat16))

def slot_gradient(illumination, propagator_phase, patches, intensity, cosine_table, sine_table):
    light_real = illumination[0]
    light_imag = illumination[1]
    spread_real = jnp.cos(propagator_phase)
    spread_imag = jnp.sin(propagator_phase)
    first_real = patches[:, 0].astype(jnp.float32)
    first_imag = patches[:, 1].astype(jnp.float32)
    second_real = patches[:, 2].astype(jnp.float32)
    second_imag = patches[:, 3].astype(jnp.float32)
    wave_real, wave_imag = to_half(complex_product(light_real, light_imag, first_real, first_imag))
    front_real, front_imag = transform(wave_real, wave_imag, 1.0, cosine_table, sine_table)
    mixed_real, mixed_imag = to_half(complex_product(spread_real, spread_imag, front_real, front_imag))
    passed_real, passed_imag = transform(mixed_real, mixed_imag, -1.0, cosine_table, sine_table)
    wave2_real, wave2_imag = to_half(complex_product(passed_real, passed_imag, second_real, second_imag))
    far_real, far_imag = transform(wave2_real, wave2_imag, 1.0, cosine_table, sine_table)
    misfit = far_real * far_real + far_imag * far_imag - intensity.astype(jnp.float32)
    pull_real = (misfit * far_real).astype(jnp.bfloat16)
    pull_imag = (misfit * far_imag).astype(jnp.bfloat16)
    back_real, back_imag = transform(pull_real, pull_imag, -1.0, cosine_table, sine_table)
    grad2_real, grad2_imag = to_half(complex_product(passed_real, -passed_imag, back_real, back_imag))
    inward_real, inward_imag = to_half(complex_product(second_real, -second_imag, back_real, back_imag))
    lifted_real, lifted_imag = transform(inward_real, inward_imag, 1.0, cosine_table, sine_table)
    reverted_real, reverted_imag = to_half(complex_product(spread_real, -spread_imag, lifted_real, lifted_imag))
    start_real, start_imag = transform(reverted_real, reverted_imag, -1.0, cosine_table, sine_table)
    grad1_real, grad1_imag = to_half(complex_product(light_real, -light_imag, start_real, start_imag))
    return jnp.stack([grad1_real, grad1_imag, grad2_real, grad2_imag], axis=1)

def reference(objects, illumination, propagator_phase, intensity, offsets, counts):
    margin = PROBE // 2
    cosine_table, sine_table = tables(PROBE)
    padded = jnp.pad(objects.astype(jnp.bfloat16), ((0, 0), (margin, margin), (margin, margin)))
    summed = jnp.zeros(padded.shape, jnp.float32)
    block_rows = math.gcd(SLOTS, 4)
    zero_index = jnp.zeros((), jnp.int32)

    def fetch(row_at, col_at):
        return lax.dynamic_slice(padded, (zero_index, row_at, col_at), (4, PROBE, PROBE))

    def one_block(block_id, summed):
        first = block_id.astype(jnp.int32) * block_rows
        number = first + jnp.arange(block_rows, dtype=jnp.int32)
        device = number // SLOTS
        slot_ids = number % SLOTS
        row_ids = device // N_COL
        col_ids = device % N_COL
        corners = lax.dynamic_slice_in_dim(offsets, first, block_rows, 0)
        start_row = (row_ids * TILE + (corners[:, 0] + 1) * margin).astype(jnp.int32)
        start_col = (col_ids * TILE + (corners[:, 1] + 1) * margin).astype(jnp.int32)
        live = slot_ids < counts[device]
        patches = jax.vmap(fetch)(start_row, start_col)
        measured = lax.dynamic_slice_in_dim(intensity, first, block_rows, 0)
        results = slot_gradient(illumination, propagator_phase, patches, measured, cosine_table, sine_table)
        results = jnp.where(live[:, None, None, None], results.astype(jnp.float32), jnp.zeros((), jnp.float32))
        for member in range(block_rows):
            where_at = (zero_index, start_row[member], start_col[member])
            window = lax.dynamic_slice(summed, where_at, (4, PROBE, PROBE))
            summed = lax.dynamic_update_slice(summed, window + results[member], where_at)
        return summed
    summed = lax.fori_loop(0, TASKS // block_rows, one_block, summed)
    return summed[:, margin:-margin, margin:-margin]
```

```python
import functools
import math

import jax
import jax.numpy as jnp
from jax import lax
from jax.experimental import pallas as pl
from jax.experimental.pallas import tpu as pltpu
from jax.sharding import PartitionSpec as P

EXTENT = 256
HALF = EXTENT // 2
CHUNK = 64


def from_behind(x, axis, by):
    size = lax.axis_size(axis)
    pairs = [(i, i + by) for i in range(size) if 0 <= i + by < size]
    return lax.ppermute(x, axis, pairs)


def extended_2(x, sides, width):
    for axis, dim in sides:
        size, length = (lax.axis_size(axis), x.shape[dim])
        up = [(i, (i + 1) % size) for i in range(size - 1)]
        down = [(j, i) for i, j in up]
        last = lax.slice_in_dim(x, length - width, length, axis=dim)
        initial = lax.slice_in_dim(x, 0, width, axis=dim)
        before = lax.ppermute(last, axis, up)
        after = lax.ppermute(initial, axis, down)
        x = jnp.concatenate([before, x, after], axis=dim)
    return x


def tables(extent):
    number = jnp.arange(extent, dtype=jnp.int32)
    turns = number[:, None] * number[None, :] % extent
    angle = turns.astype(jnp.float32) * (2.0 * math.pi / extent)
    scale = 1.0 / math.sqrt(extent)
    cosine = (jnp.cos(angle) * scale).astype(jnp.bfloat16)
    sine = (jnp.sin(angle) * scale).astype(jnp.bfloat16)
    forward = jnp.block([[cosine, sine], [-sine, cosine]])
    inverse = jnp.block([[cosine, -sine], [sine, cosine]])
    return forward, inverse


def chunks(body):
    for r in range(0, EXTENT, CHUNK):
        body(pl.ds(r, CHUNK))


def transform(field, upper, out, left, right):
    u = jnp.dot(left[...], field[...], preferred_element_type=jnp.float32)
    upper[:, :EXTENT] = u[:EXTENT].astype(jnp.bfloat16)
    upper[:, EXTENT:] = u[EXTENT:].astype(jnp.bfloat16)
    out[...] = jnp.dot(upper[...], right[...], preferred_element_type=jnp.float32)


def slot_kernel(
    meta, count, intensity, light, spread, forward, inverse, ext, summed,
    field, upper, out, passed, acc, measured, sems,
):
    number = count[0]

    def fetch(i, buf):
        return pltpu.make_async_copy(intensity.at[meta[0, i]], measured.at[buf], sems.at[buf])

    @pl.when(number > 0)
    def _():
        fetch(0, 0).start()

    acc[...] = jnp.zeros_like(acc)

    def one(i, carry):
        buf = lax.rem(i, 2)
        fetch(i, buf).wait()

        @pl.when(i + 1 < number)
        def _():
            fetch(i + 1, 1 - buf).start()

        row = pl.multiple_of(meta[1, i] * HALF, HALF)
        col = pl.multiple_of(meta[2, i] * HALF, HALF)
        cols = pl.ds(col, EXTENT)

        def patch(plane, rows):
            at = pl.ds(pl.multiple_of(row + rows.start, CHUNK), CHUNK)
            return ext[plane, at, cols].astype(jnp.float32)

        def put(rows, real, imag):
            field[rows, :] = real.astype(jnp.bfloat16)
            field[pl.ds(rows.start + EXTENT, CHUNK), :] = imag.astype(jnp.bfloat16)

        def add(plane, rows, value):
            at = pl.ds(pl.multiple_of(row + rows.start, CHUNK), CHUNK)
            acc[plane, at, cols] += value

        def wave(rows):
            a, b = patch(0, rows), patch(1, rows)
            p, q = light[0, rows, :], light[1, rows, :]
            put(rows, p * a - q * b, p * b + q * a)

        chunks(wave)
        transform(field, upper, out, forward, inverse)

        def mix(rows):
            a, b = out[rows, :EXTENT], out[rows, EXTENT:]
            p, q = spread[0, rows, :], spread[1, rows, :]
            put(rows, p * a - q * b, p * b + q * a)

        chunks(mix)
        transform(field, upper, passed, inverse, forward)

        def second(rows):
            a, b = passed[rows, :EXTENT], passed[rows, EXTENT:]
            p, q = patch(2, rows), patch(3, rows)
            put(rows, p * a - q * b, p * b + q * a)

        chunks(second)
        transform(field, upper, out, forward, inverse)

        def pull(rows):
            a, b = out[rows, :EXTENT], out[rows, EXTENT:]
            misfit = a * a + b * b - measured[buf, rows, :].astype(jnp.float32)
            put(rows, misfit * a, misfit * b)

        chunks(pull)
        transform(field, upper, out, inverse, forward)

        def inward(rows):
            a, b = out[rows, :EXTENT], out[rows, EXTENT:]
            p, q = patch(2, rows), patch(3, rows)
            put(rows, p * a + q * b, p * b - q * a)
            p, q = passed[rows, :EXTENT], passed[rows, EXTENT:]
            add(2, rows, p * a + q * b)
            add(3, rows, p * b - q * a)

        chunks(inward)
        transform(field, upper, out, forward, inverse)

        def revert(rows):
            a, b = out[rows, :EXTENT], out[rows, EXTENT:]
            p, q = spread[0, rows, :], spread[1, rows, :]
            put(rows, p * a + q * b, p * b - q * a)

        chunks(revert)
        transform(field, upper, out, inverse, forward)

        def first(rows):
            a, b = out[rows, :EXTENT], out[rows, EXTENT:]
            p, q = light[0, rows, :], light[1, rows, :]
            add(0, rows, p * a + q * b)
            add(1, rows, p * b - q * a)

        chunks(first)
        return carry

    lax.fori_loop(0, number, one, 0)
    summed[...] = acc[...]


def run_slots(meta, count, intensity, light, spread, forward, inverse, ext):
    smem = pl.BlockSpec(memory_space=pltpu.SMEM)
    vmem = pl.BlockSpec(memory_space=pltpu.VMEM)
    return pl.pallas_call(
        slot_kernel,
        out_shape=jax.ShapeDtypeStruct(ext.shape, jnp.float32),
        in_specs=[smem, smem, pl.BlockSpec(memory_space=pl.ANY)] + [vmem] * 5,
        out_specs=vmem,
        scratch_shapes=[
            pltpu.VMEM((2 * EXTENT, EXTENT), jnp.bfloat16),
            pltpu.VMEM((EXTENT, 2 * EXTENT), jnp.bfloat16),
            pltpu.VMEM((EXTENT, 2 * EXTENT), jnp.float32),
            pltpu.VMEM((EXTENT, 2 * EXTENT), jnp.float32),
            pltpu.VMEM(ext.shape, jnp.float32),
            pltpu.VMEM((2, EXTENT, EXTENT), jnp.bfloat16),
            pltpu.SemaphoreType.DMA((2,)),
        ],
        compiler_params=pltpu.CompilerParams(vmem_limit_bytes=60 * 2**20),
        cost_estimate=pl.CostEstimate(flops=12 * 48 * 2**25, bytes_accessed=2**24, transcendentals=0),
    )(meta, count, intensity, light, spread, forward, inverse, ext)


def fold_rows(summed, margin):
    top_strip = summed[:, :margin, :]
    bottom_strip = summed[:, -margin:, :]
    from_below = from_behind(top_strip.astype(jnp.bfloat16), "row", -1).astype(top_strip.dtype)
    from_above = from_behind(bottom_strip.astype(jnp.bfloat16), "row", 1).astype(bottom_strip.dtype)
    interior = summed[:, margin:-margin, :]
    interior = interior.at[:, -margin:, :].add(from_below)
    return interior.at[:, :margin, :].add(from_above)


def fold_cols(summed, margin):
    left_strip = summed[:, :, :margin]
    right_strip = summed[:, :, -margin:]
    from_right = from_behind(left_strip.astype(jnp.bfloat16), "col", -1).astype(left_strip.dtype)
    from_left = from_behind(right_strip.astype(jnp.bfloat16), "col", 1).astype(right_strip.dtype)
    interior = summed[:, :, margin:-margin]
    interior = interior.at[:, :, -margin:].add(from_right)
    return interior.at[:, :, :margin].add(from_left)


def per_device(objects, illumination, propagator_phase, intensity, offsets, counts):
    slot_count = intensity.shape[0]
    forward, inverse = tables(EXTENT)
    spread = jnp.stack([jnp.cos(propagator_phase), jnp.sin(propagator_phase)])
    rounded = objects.astype(jnp.bfloat16)
    extended = extended_2(rounded, (("row", 1), ("col", 2)), HALF)
    ids = jnp.arange(slot_count, dtype=jnp.int32)
    meta = jnp.stack([ids, offsets[:, 0] + 1, offsets[:, 1] + 1])
    summed = run_slots(meta, counts, intensity, illumination, spread, forward, inverse, extended)
    return fold_rows(fold_cols(summed, HALF), HALF)


def solution(mesh):
    placed = (
        P(None, "row", "col"),
        P(),
        P(),
        P(("row", "col"), None, None),
        P(("row", "col"), None),
        P(("row", "col")),
    )
    return jax.shard_map(
        per_device, mesh=mesh, in_specs=placed, out_specs=P(None, "row", "col"), check_vma=False
    )
```

```python
import math

import jax
import jax.numpy as jnp
import numpy as np
from jax import lax
from jax.experimental import pallas as pl
from jax.experimental.pallas import tpu as pltpu
from jax.sharding import PartitionSpec as P

EXTENT = 256
HALF = EXTENT // 2
CHUNK = 64
MESH = pl.DeviceIdType.MESH


def tables(extent):
    number = np.arange(extent, dtype=np.int32)
    turns = number[:, None] * number[None, :] % extent
    angle = turns.astype(np.float32) * np.float32(2.0 * math.pi / extent)
    scale = np.float32(1.0 / math.sqrt(extent))
    cosine = (np.cos(angle) * scale).astype(jnp.bfloat16)
    sine = (np.sin(angle) * scale).astype(jnp.bfloat16)
    forward = np.block([[cosine, sine], [-sine, cosine]])
    inverse = np.block([[cosine, -sine], [sine, cosine]])
    return jnp.asarray(forward), jnp.asarray(inverse)


class Place:
    def __init__(self):
        r, c = lax.axis_index("row"), lax.axis_index("col")
        self.has_above, self.has_below = r > 0, r < lax.axis_size("row") - 1
        self.has_left, self.has_right = c > 0, c < lax.axis_size("col") - 1
        self.above, self.below = (r - 1, c), (r + 1, c)
        self.left, self.right = (r, c - 1), (r, c + 1)
        self.sides = (
            (self.has_above, self.above),
            (self.has_below, self.below),
            (self.has_left, self.left),
            (self.has_right, self.right),
        )

    def greet(self):
        barrier = pltpu.get_barrier_semaphore()
        for there, device in self.sides:
            @pl.when(there)
            def _(device=device):
                pl.semaphore_signal(barrier, inc=1, device_id=device, device_id_type=MESH)

        pl.semaphore_wait(barrier, sum(there.astype(jnp.int32) for there, _ in self.sides))


class Sends:
    def __init__(self, send, recv):
        self.send, self.recv, self.all = send, recv, {}

    def add(self, key, source, target, device, sent, received):
        k = len(self.all)
        copy = pltpu.make_async_remote_copy(
            src_ref=source, dst_ref=target, send_sem=self.send.at[k], recv_sem=self.recv.at[k],
            device_id=device, device_id_type=MESH,
        )
        self.all[key] = (copy, sent, received)

    def start(self, *keys):
        for key in keys:
            copy, sent, _ = self.all[key]
            pl.when(sent)(copy.start)

    def wait_recv(self, *keys):
        for key in keys:
            copy, _, received = self.all[key]
            pl.when(received)(copy.wait_recv)

    def wait_send(self):
        for copy, sent, _ in self.all.values():
            pl.when(sent)(copy.wait_send)


def both(a, b):
    return jnp.logical_and(a, b)


def halo_kernel(objects, phase, ext, spread, stage, loads, send, recv):
    tile = objects.shape[1]
    near, far, end = HALF, HALF + tile, 2 * HALF + tile
    own = slice(near, far)
    first, last = slice(0, near), slice(far, end)
    top, bottom = slice(near, 2 * near), slice(tile, far)
    place = Place()
    bands = ((tile - HALF, HALF), (0, HALF), (HALF, tile - 2 * HALF))
    loading = [
        pltpu.make_async_copy(objects.at[:, pl.ds(at, size)], stage.at[:, pl.ds(at, size)], loads.at[k])
        for k, (at, size) in enumerate(bands)
    ]
    for copy in loading:
        copy.start()
    place.greet()

    sends = Sends(send, recv)

    def route(key, source, target, device, sent, received):
        sends.add(key, ext.at[(slice(None),) + source], ext.at[(slice(None),) + target], device, sent, received)

    middle = slice(2 * near, tile)
    for name, cols in (("l", top), ("r", bottom), ("m", middle)):
        route("down" + name, (bottom, cols), (first, cols), place.below, place.has_below, place.has_above)
        route("up" + name, (top, cols), (last, cols), place.above, place.has_above, place.has_below)
    route("right", (own, bottom), (own, first), place.right, place.has_right, place.has_left)
    route("left", (own, top), (own, last), place.left, place.has_left, place.has_right)
    for name, rows, there in (("t", first, place.has_above), ("b", last, place.has_below)):
        route("right" + name, (rows, bottom), (rows, first), place.right,
              both(place.has_right, there), both(place.has_left, there))
        route("left" + name, (rows, top), (rows, last), place.left,
              both(place.has_left, there), both(place.has_right, there))

    def cast(k):
        loading[k].wait()
        at, size = bands[k]
        for plane in range(4):
            ext[plane, near + at:near + at + size, near:far] = stage[plane, at:at + size].astype(jnp.bfloat16)

    cast(0)
    sends.start("downl", "downr")
    cast(1)
    sends.start("upl", "upr", "downm", "upm")
    cast(2)
    sends.start("right", "left")

    def blank(there, rows, cols):
        @pl.when(jnp.logical_not(there))
        def _():
            part = ext.at[:, rows, cols]
            part[...] = jnp.zeros(part.shape, jnp.bfloat16)

    blank(place.has_above, first, own)
    blank(place.has_below, last, own)
    blank(place.has_left, own, first)
    blank(place.has_right, own, last)
    for rows, there in ((first, place.has_above), (last, place.has_below)):
        blank(both(there, place.has_left), rows, first)
        blank(both(there, place.has_right), rows, last)
    spread[0] = jnp.cos(phase[...])
    spread[1] = jnp.sin(phase[...])

    sends.wait_recv("downl", "downr")
    sends.start("leftt", "rightt")
    sends.wait_recv("upl", "upr")
    sends.start("leftb", "rightb")
    sends.wait_recv("right", "left", "downm", "upm", "leftt", "rightt", "leftb", "rightb")
    sends.wait_send()


def halo(objects, phase):
    tile = objects.shape[1]
    size = tile + 2 * HALF
    vmem = pl.BlockSpec(memory_space=pltpu.VMEM)
    return pl.pallas_call(
        halo_kernel,
        out_shape=(
            pltpu.VMEM((4, size, size), jnp.bfloat16),
            pltpu.VMEM((2, EXTENT, EXTENT), jnp.float32),
        ),
        in_specs=[pl.BlockSpec(memory_space=pltpu.HBM), vmem],
        out_specs=(vmem, vmem),
        scratch_shapes=[
            pltpu.VMEM(objects.shape, jnp.float32),
            pltpu.SemaphoreType.DMA((3,)),
            pltpu.SemaphoreType.DMA((12,)),
            pltpu.SemaphoreType.DMA((12,)),
        ],
        compiler_params=pltpu.CompilerParams(
            collective_id=0, has_side_effects=True, vmem_limit_bytes=24 * 2**20
        ),
    )(pltpu.with_memory_space_constraint(objects, pltpu.HBM), phase)


def margin_kernel(
    acc, out, row_send, row_recv, col_send, col_recv, corner_send, corner_recv, send, recv
):
    tile = out.shape[1]
    near, far, end = HALF, HALF + tile, 2 * HALF + tile
    own = slice(near, far)
    edges = (slice(0, near), slice(far, end))
    inner = slice(near, tile - near)
    outer = (slice(0, near), slice(tile - near, tile))
    place = Place()
    place.greet()
    rows = ((place.has_above, place.above), (place.has_below, place.below))
    cols = ((place.has_left, place.left), (place.has_right, place.right))

    sends = Sends(send, recv)
    for side, (there, device) in enumerate(cols):
        back = cols[1 - side][0]
        sends.add(f"corner{side}", corner_send.at[side], corner_recv.at[1 - side], device, there, back)
        sends.add(f"col{side}", col_send.at[side], col_recv.at[1 - side], device, there, back)
    for side, (there, device) in enumerate(rows):
        back = rows[1 - side][0]
        for name, part in (("m", inner), ("l", outer[0]), ("r", outer[1])):
            sends.add(
                f"row{side}{name}", row_send.at[side, :, :, part], row_recv.at[1 - side, :, :, part],
                device, there, back,
            )

    for c in range(2):
        for r in range(2):
            corner_send[c, r] = acc[:, edges[r], edges[c]].astype(jnp.bfloat16)
        sends.start(f"corner{c}")
    for r in range(2):
        row_send[r, :, :, inner] = acc[:, edges[r], 2 * near:tile].astype(jnp.bfloat16)
        sends.start(f"row{r}m")
    for c in range(2):
        for plane in range(4):
            col_send[c, plane] = acc[plane, own, edges[c]].astype(jnp.bfloat16)
        sends.start(f"col{c}")

    for side in range(2):
        @pl.when(jnp.logical_not(cols[side][0]))
        def _(side=side):
            corner_recv[side] = jnp.zeros(corner_recv.shape[1:], jnp.bfloat16)
            col_recv[side] = jnp.zeros(col_recv.shape[1:], jnp.bfloat16)

        @pl.when(jnp.logical_not(rows[side][0]))
        def _(side=side):
            row_recv[side] = jnp.zeros(row_recv.shape[1:], jnp.bfloat16)

    sends.wait_recv("corner0", "corner1")
    for r in range(2):
        for c, name in enumerate("lr"):
            at = slice(near + outer[c].start, near + outer[c].stop)
            total = acc[:, edges[r], at] + corner_recv[c, r].astype(jnp.float32)
            row_send[r, :, :, outer[c]] = total.astype(jnp.bfloat16)
            sends.start(f"row{r}{name}")

    for plane in range(4):
        out[plane] = acc[plane, own, own]
    sends.wait_recv("col0", "col1")
    for c in range(2):
        for plane in range(4):
            out[plane, :, outer[c]] += col_recv[c, plane].astype(jnp.float32)
    sends.wait_recv("row0m", "row1m", "row0l", "row1l", "row0r", "row1r")
    for r in range(2):
        for plane in range(4):
            out[plane, outer[r], :] += row_recv[r, plane].astype(jnp.float32)
    sends.wait_send()


def margins(acc, tile):
    vmem = pl.BlockSpec(memory_space=pltpu.VMEM)
    row = pltpu.VMEM((2, 4, HALF, tile), jnp.bfloat16)
    col = pltpu.VMEM((2, 4, tile, HALF), jnp.bfloat16)
    corner = pltpu.VMEM((2, 2, 4, HALF, HALF), jnp.bfloat16)
    return pl.pallas_call(
        margin_kernel,
        out_shape=pltpu.VMEM((4, tile, tile), jnp.float32),
        in_specs=[vmem],
        out_specs=vmem,
        scratch_shapes=[
            row, row, col, col, corner, corner,
            pltpu.SemaphoreType.DMA((10,)),
            pltpu.SemaphoreType.DMA((10,)),
        ],
        compiler_params=pltpu.CompilerParams(
            collective_id=1, has_side_effects=True, vmem_limit_bytes=32 * 2**20
        ),
    )(acc)


def chunks(body):
    for r in range(0, EXTENT, CHUNK):
        body(pl.ds(r, CHUNK))


def transform(field, upper, out, left, right):
    u = jnp.dot(left[...], field[...], preferred_element_type=jnp.float32)
    upper[:, :EXTENT] = u[:EXTENT].astype(jnp.bfloat16)
    upper[:, EXTENT:] = u[EXTENT:].astype(jnp.bfloat16)
    out[...] = jnp.dot(upper[...], right[...], preferred_element_type=jnp.float32)


def slot_kernel(
    offsets, count, intensity, light, spread, forward, inverse, ext, acc,
    field, upper, out, passed, measured, sems,
):
    number = count[0]

    def fetch(i, buf):
        return pltpu.make_async_copy(intensity.at[i], measured.at[buf], sems.at[buf])

    @pl.when(number > 0)
    def _():
        fetch(0, 0).start()

    acc[...] = jnp.zeros_like(acc)

    def one(i, carry):
        buf = lax.rem(i, 2)
        fetch(i, buf).wait()

        @pl.when(i + 1 < number)
        def _():
            fetch(i + 1, 1 - buf).start()

        row = pl.multiple_of((offsets[i, 0] + 1) * HALF, HALF)
        col = pl.multiple_of((offsets[i, 1] + 1) * HALF, HALF)
        cols = pl.ds(col, EXTENT)

        def patch(plane, rows):
            at = pl.ds(pl.multiple_of(row + rows.start, CHUNK), CHUNK)
            return ext[plane, at, cols].astype(jnp.float32)

        def put(rows, real, imag):
            field[rows, :] = real.astype(jnp.bfloat16)
            field[pl.ds(rows.start + EXTENT, CHUNK), :] = imag.astype(jnp.bfloat16)

        def add(plane, rows, value):
            at = pl.ds(pl.multiple_of(row + rows.start, CHUNK), CHUNK)
            acc[plane, at, cols] += value

        def wave(rows):
            a, b = patch(0, rows), patch(1, rows)
            p, q = light[0, rows, :], light[1, rows, :]
            put(rows, p * a - q * b, p * b + q * a)

        chunks(wave)
        transform(field, upper, out, forward, inverse)

        def mix(rows):
            a, b = out[rows, :EXTENT], out[rows, EXTENT:]
            p, q = spread[0, rows, :], spread[1, rows, :]
            put(rows, p * a - q * b, p * b + q * a)

        chunks(mix)
        transform(field, upper, passed, inverse, forward)

        def second(rows):
            a, b = passed[rows, :EXTENT], passed[rows, EXTENT:]
            p, q = patch(2, rows), patch(3, rows)
            put(rows, p * a - q * b, p * b + q * a)

        chunks(second)
        transform(field, upper, out, forward, inverse)

        def pull(rows):
            a, b = out[rows, :EXTENT], out[rows, EXTENT:]
            misfit = a * a + b * b - measured[buf, rows, :].astype(jnp.float32)
            put(rows, misfit * a, misfit * b)

        chunks(pull)
        transform(field, upper, out, inverse, forward)

        def inward(rows):
            a, b = out[rows, :EXTENT], out[rows, EXTENT:]
            p, q = patch(2, rows), patch(3, rows)
            put(rows, p * a + q * b, p * b - q * a)
            p, q = passed[rows, :EXTENT], passed[rows, EXTENT:]
            add(2, rows, p * a + q * b)
            add(3, rows, p * b - q * a)

        chunks(inward)
        transform(field, upper, out, forward, inverse)

        def revert(rows):
            a, b = out[rows, :EXTENT], out[rows, EXTENT:]
            p, q = spread[0, rows, :], spread[1, rows, :]
            put(rows, p * a + q * b, p * b - q * a)

        chunks(revert)
        transform(field, upper, out, inverse, forward)

        def first(rows):
            a, b = out[rows, :EXTENT], out[rows, EXTENT:]
            p, q = light[0, rows, :], light[1, rows, :]
            add(0, rows, p * a + q * b)
            add(1, rows, p * b - q * a)

        chunks(first)
        return carry

    lax.fori_loop(0, number, one, 0)


def run_slots(offsets, count, intensity, light, spread, forward, inverse, ext):
    smem = pl.BlockSpec(memory_space=pltpu.SMEM)
    vmem = pl.BlockSpec(memory_space=pltpu.VMEM)
    return pl.pallas_call(
        slot_kernel,
        out_shape=pltpu.VMEM(ext.shape, jnp.float32),
        in_specs=[smem, smem, pl.BlockSpec(memory_space=pltpu.HBM)] + [vmem] * 5,
        out_specs=vmem,
        scratch_shapes=[
            pltpu.VMEM((2 * EXTENT, EXTENT), jnp.bfloat16),
            pltpu.VMEM((EXTENT, 2 * EXTENT), jnp.bfloat16),
            pltpu.VMEM((EXTENT, 2 * EXTENT), jnp.float32),
            pltpu.VMEM((EXTENT, 2 * EXTENT), jnp.float32),
            pltpu.VMEM((2, EXTENT, EXTENT), jnp.bfloat16),
            pltpu.SemaphoreType.DMA((2,)),
        ],
        compiler_params=pltpu.CompilerParams(vmem_limit_bytes=14 * 2**20),
        cost_estimate=pl.CostEstimate(flops=12 * 48 * 2**25, bytes_accessed=2**24, transcendentals=0),
    )(offsets, count, intensity, light, spread, forward, inverse, ext)


def per_device(objects, illumination, propagator_phase, intensity, offsets, counts):
    forward, inverse = tables(EXTENT)
    ext, spread = halo(objects, propagator_phase)
    acc = run_slots(offsets, counts, intensity, illumination, spread, forward, inverse, ext)
    return margins(acc, objects.shape[1])


def solution(mesh):
    placed = (
        P(None, "row", "col"),
        P(),
        P(),
        P(("row", "col"), None, None),
        P(("row", "col"), None),
        P(("row", "col")),
    )
    return jax.shard_map(
        per_device, mesh=mesh, in_specs=placed, out_specs=P(None, "row", "col"), check_vma=False
    )
```

```python
import math

import jax
import jax.numpy as jnp
import numpy as np
from jax import lax
from jax.experimental import pallas as pl
from jax.experimental.pallas import tpu as pltpu
from jax.sharding import PartitionSpec as P

EXTENT = 256
HALF = EXTENT // 2
MESH = pl.DeviceIdType.MESH


def tables(extent):
    half = extent // 2
    number = np.arange(extent, dtype=np.int32)
    turns = number[:, None] * number[None, :] % extent
    angle = turns.astype(np.float32) * np.float32(2.0 * math.pi / extent)
    scale = np.float32(1.0 / math.sqrt(extent))
    cosine = (np.cos(angle) * scale).astype(jnp.bfloat16)
    sine = (np.sin(angle) * scale).astype(jnp.bfloat16)
    folded = np.concatenate([cosine[:, : half + 1], sine[:, 1:half]], axis=1)
    order = np.concatenate([number[: half + 1], extent - number[1:half]])
    pick = np.eye(extent, dtype=np.float32)[order].astype(jnp.bfloat16)
    return tuple(jnp.asarray(np.ascontiguousarray(x)) for x in (folded, folded.T, pick, pick.T))


def product(a, b):
    return jnp.dot(a, b, preferred_element_type=jnp.float32)


def half(x):
    return x.astype(jnp.bfloat16)


class Place:
    def __init__(self):
        r, c = lax.axis_index("row"), lax.axis_index("col")
        self.has_above, self.has_below = r > 0, r < lax.axis_size("row") - 1
        self.has_left, self.has_right = c > 0, c < lax.axis_size("col") - 1
        self.above, self.below = (r - 1, c), (r + 1, c)
        self.left, self.right = (r, c - 1), (r, c + 1)
        self.sides = (
            (self.has_above, self.above),
            (self.has_below, self.below),
            (self.has_left, self.left),
            (self.has_right, self.right),
        )

    def greet(self):
        barrier = pltpu.get_barrier_semaphore()
        for there, device in self.sides:
            @pl.when(there)
            def _(device=device):
                pl.semaphore_signal(barrier, inc=1, device_id=device, device_id_type=MESH)

        pl.semaphore_wait(barrier, sum(there.astype(jnp.int32) for there, _ in self.sides))


class Sends:
    def __init__(self, send, recv):
        self.send, self.recv, self.all = send, recv, {}

    def add(self, key, source, target, device, sent, received):
        k = len(self.all)
        copy = pltpu.make_async_remote_copy(
            src_ref=source, dst_ref=target, send_sem=self.send.at[k], recv_sem=self.recv.at[k],
            device_id=device, device_id_type=MESH,
        )
        self.all[key] = (copy, sent, received)

    def start(self, *keys):
        for key in keys:
            copy, sent, _ = self.all[key]
            pl.when(sent)(copy.start)

    def wait_recv(self, *keys):
        for key in keys:
            copy, _, received = self.all[key]
            pl.when(received)(copy.wait_recv)

    def wait_send(self):
        for copy, sent, _ in self.all.values():
            pl.when(sent)(copy.wait_send)


def both(a, b):
    return jnp.logical_and(a, b)


def halo_kernel(objects, phase, pick, pick_t, ext, spread, stage, loads, send, recv):
    tile = objects.shape[1]
    near, far, end = HALF, HALF + tile, 2 * HALF + tile
    own = slice(near, far)
    first, last = slice(0, near), slice(far, end)
    top, bottom = slice(near, 2 * near), slice(tile, far)
    place = Place()
    bands = ((tile - HALF, HALF), (0, HALF), (HALF, tile - 2 * HALF))
    loading = [
        pltpu.make_async_copy(objects.at[:, pl.ds(at, size)], stage.at[:, pl.ds(at, size)], loads.at[k])
        for k, (at, size) in enumerate(bands)
    ]
    for copy in loading:
        copy.start()
    place.greet()

    sends = Sends(send, recv)

    def route(key, source, target, device, sent, received):
        sends.add(key, ext.at[(slice(None),) + source], ext.at[(slice(None),) + target], device, sent, received)

    middle = slice(2 * near, tile)
    for name, cols in (("l", top), ("r", bottom), ("m", middle)):
        route("down" + name, (bottom, cols), (first, cols), place.below, place.has_below, place.has_above)
        route("up" + name, (top, cols), (last, cols), place.above, place.has_above, place.has_below)
    route("right", (own, bottom), (own, first), place.right, place.has_right, place.has_left)
    route("left", (own, top), (own, last), place.left, place.has_left, place.has_right)
    for name, rows, there in (("t", first, place.has_above), ("b", last, place.has_below)):
        route("right" + name, (rows, bottom), (rows, first), place.right,
              both(place.has_right, there), both(place.has_left, there))
        route("left" + name, (rows, top), (rows, last), place.left,
              both(place.has_left, there), both(place.has_right, there))

    def cast(k):
        loading[k].wait()
        at, size = bands[k]
        for plane in range(4):
            ext[plane, near + at:near + at + size, near:far] = stage[plane, at:at + size].astype(jnp.bfloat16)

    cast(0)
    sends.start("downl", "downr")
    cast(1)
    sends.start("upl", "upr", "downm", "upm")
    cast(2)
    sends.start("right", "left")

    def blank(there, rows, cols):
        @pl.when(jnp.logical_not(there))
        def _():
            part = ext.at[:, rows, cols]
            part[...] = jnp.zeros(part.shape, jnp.bfloat16)

    blank(place.has_above, first, own)
    blank(place.has_below, last, own)
    blank(place.has_left, own, first)
    blank(place.has_right, own, last)
    for rows, there in ((first, place.has_above), (last, place.has_below)):
        blank(both(there, place.has_left), rows, first)
        blank(both(there, place.has_right), rows, last)
    rest, ordered = phase[...], 0.0
    for _ in range(3):
        part = half(rest)
        rest = rest - part.astype(jnp.float32)
        ordered = ordered + product(half(product(pick[...], part)), pick_t[...])
    spread[0] = jnp.cos(ordered)
    spread[1] = jnp.sin(ordered)

    sends.wait_recv("downl", "downr")
    sends.start("leftt", "rightt")
    sends.wait_recv("upl", "upr")
    sends.start("leftb", "rightb")
    sends.wait_recv("right", "left", "downm", "upm", "leftt", "rightt", "leftb", "rightb")
    sends.wait_send()


def halo(objects, phase, pick, pick_t):
    tile = objects.shape[1]
    size = tile + 2 * HALF
    vmem = pl.BlockSpec(memory_space=pltpu.VMEM)
    return pl.pallas_call(
        halo_kernel,
        out_shape=(
            pltpu.VMEM((4, size, size), jnp.bfloat16),
            pltpu.VMEM((2, EXTENT, EXTENT), jnp.float32),
        ),
        in_specs=[pl.BlockSpec(memory_space=pltpu.HBM), vmem, vmem, vmem],
        out_specs=(vmem, vmem),
        scratch_shapes=[
            pltpu.VMEM(objects.shape, jnp.float32),
            pltpu.SemaphoreType.DMA((3,)),
            pltpu.SemaphoreType.DMA((12,)),
            pltpu.SemaphoreType.DMA((12,)),
        ],
        compiler_params=pltpu.CompilerParams(
            collective_id=0, has_side_effects=True, vmem_limit_bytes=24 * 2**20
        ),
    )(pltpu.with_memory_space_constraint(objects, pltpu.HBM), phase, pick, pick_t)


def margin_kernel(
    acc, out, row_send, row_recv, col_send, col_recv, corner_send, corner_recv, send, recv
):
    tile = out.shape[1]
    near, far, end = HALF, HALF + tile, 2 * HALF + tile
    own = slice(near, far)
    edges = (slice(0, near), slice(far, end))
    inner = slice(near, tile - near)
    outer = (slice(0, near), slice(tile - near, tile))
    place = Place()
    place.greet()
    rows = ((place.has_above, place.above), (place.has_below, place.below))
    cols = ((place.has_left, place.left), (place.has_right, place.right))

    sends = Sends(send, recv)
    for side, (there, device) in enumerate(cols):
        back = cols[1 - side][0]
        sends.add(f"corner{side}", corner_send.at[side], corner_recv.at[1 - side], device, there, back)
        sends.add(f"col{side}", col_send.at[side], col_recv.at[1 - side], device, there, back)
    for side, (there, device) in enumerate(rows):
        back = rows[1 - side][0]
        for name, part in (("m", inner), ("l", outer[0]), ("r", outer[1])):
            sends.add(
                f"row{side}{name}", row_send.at[side, :, :, part], row_recv.at[1 - side, :, :, part],
                device, there, back,
            )

    for c in range(2):
        for r in range(2):
            corner_send[c, r] = acc[:, edges[r], edges[c]].astype(jnp.bfloat16)
        sends.start(f"corner{c}")
    for r in range(2):
        row_send[r, :, :, inner] = acc[:, edges[r], 2 * near:tile].astype(jnp.bfloat16)
        sends.start(f"row{r}m")
    for c in range(2):
        for plane in range(4):
            col_send[c, plane] = acc[plane, own, edges[c]].astype(jnp.bfloat16)
        sends.start(f"col{c}")

    for side in range(2):
        @pl.when(jnp.logical_not(cols[side][0]))
        def _(side=side):
            corner_recv[side] = jnp.zeros(corner_recv.shape[1:], jnp.bfloat16)
            col_recv[side] = jnp.zeros(col_recv.shape[1:], jnp.bfloat16)

        @pl.when(jnp.logical_not(rows[side][0]))
        def _(side=side):
            row_recv[side] = jnp.zeros(row_recv.shape[1:], jnp.bfloat16)

    sends.wait_recv("corner0", "corner1")
    for r in range(2):
        for c, name in enumerate("lr"):
            at = slice(near + outer[c].start, near + outer[c].stop)
            total = acc[:, edges[r], at] + corner_recv[c, r].astype(jnp.float32)
            row_send[r, :, :, outer[c]] = total.astype(jnp.bfloat16)
            sends.start(f"row{r}{name}")

    for plane in range(4):
        out[plane] = acc[plane, own, own]
    sends.wait_recv("col0", "col1")
    for c in range(2):
        for plane in range(4):
            out[plane, :, outer[c]] += col_recv[c, plane].astype(jnp.float32)
    sends.wait_recv("row0m", "row1m", "row0l", "row1l", "row0r", "row1r")
    for r in range(2):
        for plane in range(4):
            out[plane, outer[r], :] += row_recv[r, plane].astype(jnp.float32)
    sends.wait_send()


def margins(acc, tile):
    vmem = pl.BlockSpec(memory_space=pltpu.VMEM)
    row = pltpu.VMEM((2, 4, HALF, tile), jnp.bfloat16)
    col = pltpu.VMEM((2, 4, tile, HALF), jnp.bfloat16)
    corner = pltpu.VMEM((2, 2, 4, HALF, HALF), jnp.bfloat16)
    return pl.pallas_call(
        margin_kernel,
        out_shape=pltpu.VMEM((4, tile, tile), jnp.float32),
        in_specs=[vmem],
        out_specs=vmem,
        scratch_shapes=[
            row, row, col, col, corner, corner,
            pltpu.SemaphoreType.DMA((10,)),
            pltpu.SemaphoreType.DMA((10,)),
        ],
        compiler_params=pltpu.CompilerParams(
            collective_id=1, has_side_effects=True, vmem_limit_bytes=32 * 2**20
        ),
    )(acc)


def output_fold(a, b, first):
    (ca, sa), (cb, sb) = a, b
    if first is None:
        return (ca + sb, cb - sa), (ca - sb, cb + sa)
    sa0, sb0 = jnp.where(first, 0.0, sa), jnp.where(first, 0.0, sb)
    low, high = jnp.where(first, sa, ca), jnp.where(first, sb, cb)
    return (ca + sb0, cb - sa0), (low - sb0, high + sa0)


def input_fold(top, bottom, first):
    (tr, ti), (br, bi) = top, bottom
    if first is None:
        return (tr + br, bi - ti), (ti + bi, tr - br)
    br0, bi0 = jnp.where(first, 0.0, br), jnp.where(first, 0.0, bi)
    return (tr + br0, jnp.where(first, br, bi - ti)), (ti + bi0, jnp.where(first, bi, tr - br))


def times(a, b):
    return a[0] * b[0] - a[1] * b[1], a[0] * b[1] + a[1] * b[0]


def conj_times(a, b):
    return a[0] * b[0] + a[1] * b[1], a[0] * b[1] - a[1] * b[0]


ROWS = 32
FULL = tuple(slice(r, r + ROWS) for r in range(0, EXTENT, ROWS))
UPPER = FULL[: len(FULL) // 2]
LEFT, RIGHT = slice(0, HALF), slice(HALF, EXTENT)


def one_slot(k, live, row, col, light, spread, table, table_t, pick, pick_t, ext, acc, measured,
             field, upper, folded, passed, ordered):
    cols = pl.ds(pl.multiple_of(col * HALF, HALF), EXTENT)
    lane = lax.broadcasted_iota(jnp.int32, (ROWS, HALF), 1) == 0
    top_row = lax.broadcasted_iota(jnp.int32, (ROWS, EXTENT), 0) == 0

    def place(rows):
        return pl.ds(pl.multiple_of(row * HALF + rows.start, ROWS), ROWS)

    def patch(plane, rows):
        at = place(rows)
        return tuple(ext[plane + i, at, cols].astype(jnp.float32) for i in range(2))

    def pair(ref, rows):
        return ref[0, rows, :], ref[1, rows, :]

    def put(ref, rows, value, columns=slice(None)):
        ref[0, rows, columns] = half(value[0])
        ref[1, rows, columns] = half(value[1])

    def add(plane, rows, value):
        at = place(rows)
        for i in range(2):
            acc[plane + i, at, cols] += value[i]

    def wave():
        for rows in FULL:
            put(field, rows, times(pair(light, rows), patch(0, rows)))
        ordered[...] = half(product(pick[...], measured[...]))

    def across():
        a, b = product(field[0], table[...]), product(field[1], table[...])
        for rows in FULL:
            low, high = output_fold(
                (a[rows, LEFT], a[rows, RIGHT]), (b[rows, LEFT], b[rows, RIGHT]), lane
            )
            put(upper, rows, low, LEFT)
            put(upper, rows, high, RIGHT)

    def frequency(act):
        def run():
            a, b = product(table_t[...], upper[0]), product(table_t[...], upper[1])
            for rows in UPPER:
                lower = slice(rows.start + HALF, rows.stop + HALF)
                first = top_row if rows.start == 0 else None
                low, high = output_fold((a[rows], a[lower]), (b[rows], b[lower]), first)
                x, y = input_fold(act(low, rows), act(high, lower), first)
                folded[0, rows, :], folded[0, lower, :] = half(x[0]), half(x[1])
                folded[1, rows, :], folded[1, lower, :] = half(y[0]), half(y[1])
        return run

    def down():
        a, b = product(table[...], folded[0]), product(table[...], folded[1])
        for rows in FULL:
            x, y = input_fold(
                (a[rows, LEFT], b[rows, LEFT]), (a[rows, RIGHT], b[rows, RIGHT]), lane
            )
            upper[0, rows, LEFT], upper[0, rows, RIGHT] = half(x[0]), half(x[1])
            upper[1, rows, LEFT], upper[1, rows, RIGHT] = half(y[0]), half(y[1])

    def space(act):
        def run():
            a, b = product(upper[0], table_t[...]), product(upper[1], table_t[...])
            for rows in FULL:
                act((a[rows], b[rows]), rows)
        return run

    def mix(value, rows):
        return times(pair(spread, rows), value)

    def revert(value, rows):
        return conj_times(pair(spread, rows), value)

    def second(value, rows):
        passed[0, rows, :], passed[1, rows, :] = value
        put(field, rows, times(value, patch(2, rows)))

    def pull():
        intensity = product(ordered[...], pick_t[...])

        def act(value, rows):
            misfit = value[0] * value[0] + value[1] * value[1] - intensity[rows]
            if live is not None:
                misfit = misfit * live
            return misfit * value[0], misfit * value[1]

        frequency(act)()

    def inward(value, rows):
        put(field, rows, conj_times(patch(2, rows), value))
        add(2, rows, conj_times(pair(passed, rows), value))

    def first(value, rows):
        add(0, rows, conj_times(pair(light, rows), value))

    return (
        wave, across, frequency(mix), down, space(second),
        across, pull, down, space(inward),
        across, frequency(revert), down, space(first),
    )


def slot_kernel(
    offsets, count, intensity, light, spread, table, table_t, pick, pick_t, ext, acc,
    measured, field, upper, folded, passed, ordered, sems,
):
    number = count[0]
    steps = lax.div(number + 1, 2)

    def fetch(i, buf):
        return pltpu.make_async_copy(
            intensity.at[pl.ds(2 * i, 2)], measured.at[buf], sems.at[buf]
        )

    @pl.when(steps > 0)
    def _():
        fetch(0, 0).start()

    acc[...] = jnp.zeros_like(acc)

    def one(i, carry):
        buf = lax.rem(i, 2)
        fetch(i, buf).wait()

        @pl.when(i + 1 < steps)
        def _():
            fetch(i + 1, 1 - buf).start()

        live = (2 * i + 1 < number).astype(jnp.float32)
        stages = [
            one_slot(
                k, live if k else None, offsets[2 * i + k, 0] + 1, offsets[2 * i + k, 1] + 1,
                light, spread, table, table_t, pick, pick_t, ext, acc, measured.at[buf, k],
                field.at[k], upper.at[k], folded.at[k], passed.at[k], ordered.at[k],
            )
            for k in range(2)
        ]
        for together in zip(*stages):
            for stage in together:
                stage()
        return carry

    lax.fori_loop(0, steps, one, 0)


def run_slots(offsets, count, intensity, light, spread, constants, ext):
    smem = pl.BlockSpec(memory_space=pltpu.SMEM)
    vmem = pl.BlockSpec(memory_space=pltpu.VMEM)
    return pl.pallas_call(
        slot_kernel,
        out_shape=pltpu.VMEM(ext.shape, jnp.float32),
        in_specs=[smem, smem, pl.BlockSpec(memory_space=pltpu.HBM)] + [vmem] * 7,
        out_specs=vmem,
        scratch_shapes=[
            pltpu.VMEM((2, 2, EXTENT, EXTENT), jnp.bfloat16),
            pltpu.VMEM((2, 2, EXTENT, EXTENT), jnp.bfloat16),
            pltpu.VMEM((2, 2, EXTENT, EXTENT), jnp.bfloat16),
            pltpu.VMEM((2, 2, EXTENT, EXTENT), jnp.bfloat16),
            pltpu.VMEM((2, 2, EXTENT, EXTENT), jnp.float32),
            pltpu.VMEM((2, EXTENT, EXTENT), jnp.bfloat16),
            pltpu.SemaphoreType.DMA((2,)),
        ],
        compiler_params=pltpu.CompilerParams(vmem_limit_bytes=16 * 2**20),
        cost_estimate=pl.CostEstimate(flops=12 * 26 * 2**25, bytes_accessed=2**24, transcendentals=0),
    )(offsets, count, intensity, light, spread, *constants, ext)


def per_device(objects, illumination, propagator_phase, intensity, offsets, counts):
    constants = tables(EXTENT)
    ext, spread = halo(objects, propagator_phase, *constants[2:])
    acc = run_slots(offsets, counts, intensity, illumination, spread, constants, ext)
    return margins(acc, objects.shape[1])


def solution(mesh):
    placed = (
        P(None, "row", "col"),
        P(),
        P(),
        P(("row", "col"), None, None),
        P(("row", "col"), None),
        P(("row", "col")),
    )
    return jax.shard_map(
        per_device, mesh=mesh, in_specs=placed, out_specs=P(None, "row", "col"), check_vma=False
    )
```

```python
import math

import jax
import jax.numpy as jnp
import numpy as np
from jax import lax
from jax.experimental import pallas as pl
from jax.experimental.pallas import tpu as pltpu
from jax.sharding import PartitionSpec as P

EXTENT = 256
HALF = EXTENT // 2
MESH = pl.DeviceIdType.MESH


def tables(extent):
    half = extent // 2
    number = np.arange(extent, dtype=np.int32)
    turns = number[:, None] * number[None, :] % extent
    angle = turns.astype(np.float32) * np.float32(2.0 * math.pi / extent)
    scale = np.float32(1.0 / math.sqrt(extent))
    cosine = (np.cos(angle) * scale).astype(jnp.bfloat16)
    sine = (np.sin(angle) * scale).astype(jnp.bfloat16)
    folded = np.concatenate([cosine[:, : half + 1], sine[:, 1:half]], axis=1)
    order = np.concatenate([number[: half + 1], extent - number[1:half]])
    pick = np.eye(extent, dtype=np.float32)[order].astype(jnp.bfloat16)
    return tuple(jnp.asarray(np.ascontiguousarray(x)) for x in (folded, folded.T, pick, pick.T))


def product(a, b):
    return jnp.dot(a, b, preferred_element_type=jnp.float32)


def half(x):
    return x.astype(jnp.bfloat16)


class Place:
    def __init__(self):
        r, c = lax.axis_index("row"), lax.axis_index("col")
        self.has_above, self.has_below = r > 0, r < lax.axis_size("row") - 1
        self.has_left, self.has_right = c > 0, c < lax.axis_size("col") - 1
        self.above, self.below = (r - 1, c), (r + 1, c)
        self.left, self.right = (r, c - 1), (r, c + 1)
        self.sides = (
            (self.has_above, self.above),
            (self.has_below, self.below),
            (self.has_left, self.left),
            (self.has_right, self.right),
        )

    def greet(self):
        barrier = pltpu.get_barrier_semaphore()
        for there, device in self.sides:
            @pl.when(there)
            def _(device=device):
                pl.semaphore_signal(barrier, inc=1, device_id=device, device_id_type=MESH)

        pl.semaphore_wait(barrier, sum(there.astype(jnp.int32) for there, _ in self.sides))


class Sends:
    def __init__(self, send, recv):
        self.send, self.recv, self.all = send, recv, {}

    def add(self, key, source, target, device, sent, received):
        k = len(self.all)
        copy = pltpu.make_async_remote_copy(
            src_ref=source, dst_ref=target, send_sem=self.send.at[k], recv_sem=self.recv.at[k],
            device_id=device, device_id_type=MESH,
        )
        self.all[key] = (copy, sent, received)

    def start(self, *keys):
        for key in keys:
            copy, sent, _ = self.all[key]
            pl.when(sent)(copy.start)

    def wait_recv(self, *keys):
        for key in keys:
            copy, _, received = self.all[key]
            pl.when(received)(copy.wait_recv)

    def wait_send(self):
        for copy, sent, _ in self.all.values():
            pl.when(sent)(copy.wait_send)


def both(a, b):
    return jnp.logical_and(a, b)


def halo_kernel(
    objects, phase, pick, pick_t, ext, spread, acc, stage, angle, order, loads, send, recv
):
    tile = objects.shape[1]
    near, far, end = HALF, HALF + tile, 2 * HALF + tile
    own = slice(near, far)
    first, last = slice(0, near), slice(far, end)
    top, bottom = slice(near, 2 * near), slice(tile, far)
    place = Place()
    bands = ((tile - HALF, HALF), (0, HALF), (HALF, tile - 2 * HALF))
    loading = [
        pltpu.make_async_copy(objects.at[:, pl.ds(at, size)], stage.at[:, pl.ds(at, size)], loads.at[k])
        for k, (at, size) in enumerate(bands)
    ]
    parameters = [
        pltpu.make_async_copy(source, target, loads.at[3 + k])
        for k, (source, target) in enumerate(
            ((phase, angle), (pick, order.at[0]), (pick_t, order.at[1]))
        )
    ]
    for copy in loading + parameters:
        copy.start()
    place.greet()

    sends = Sends(send, recv)

    def route(key, source, target, device, sent, received):
        sends.add(key, ext.at[(slice(None),) + source], ext.at[(slice(None),) + target], device, sent, received)

    middle = slice(2 * near, tile)
    for name, cols in (("l", top), ("r", bottom), ("m", middle)):
        route("down" + name, (bottom, cols), (first, cols), place.below, place.has_below, place.has_above)
        route("up" + name, (top, cols), (last, cols), place.above, place.has_above, place.has_below)
    for k, (at, size) in enumerate(bands):
        rows = slice(near + at, near + at + size)
        route(f"right{k}", (rows, bottom), (rows, first), place.right, place.has_right, place.has_left)
        route(f"left{k}", (rows, top), (rows, last), place.left, place.has_left, place.has_right)
    for name, rows, there in (("t", first, place.has_above), ("b", last, place.has_below)):
        route("right" + name, (rows, bottom), (rows, first), place.right,
              both(place.has_right, there), both(place.has_left, there))
        route("left" + name, (rows, top), (rows, last), place.left,
              both(place.has_left, there), both(place.has_right, there))

    def cast(k):
        loading[k].wait()
        at, size = bands[k]
        for plane in range(4):
            ext[plane, near + at:near + at + size, near:far] = stage[plane, at:at + size].astype(jnp.bfloat16)

    cast(0)
    sends.start("downl", "downr", "right0", "left0")
    cast(1)
    sends.start("upl", "upr", "right1", "left1")
    cast(2)
    sends.start("right2", "left2", "downm", "upm")

    def blank(there, rows, cols):
        @pl.when(jnp.logical_not(there))
        def _():
            part = ext.at[:, rows, cols]
            part[...] = jnp.zeros(part.shape, jnp.bfloat16)

    blank(place.has_above, first, own)
    blank(place.has_below, last, own)
    blank(place.has_left, own, first)
    blank(place.has_right, own, last)
    for rows, there in ((first, place.has_above), (last, place.has_below)):
        blank(both(there, place.has_left), rows, first)
        blank(both(there, place.has_right), rows, last)
    for copy in parameters:
        copy.wait()
    rest, ordered = angle[...], 0.0
    for _ in range(3):
        part = half(rest)
        rest = rest - part.astype(jnp.float32)
        ordered = ordered + product(half(product(order[0], part)), order[1])
    spread[0] = jnp.cos(ordered)
    spread[1] = jnp.sin(ordered)
    for plane in range(4):
        acc[plane] = jnp.zeros(acc.shape[1:], jnp.float32)

    sends.wait_recv("downl", "downr")
    sends.start("leftt", "rightt")
    sends.wait_recv("upl", "upr")
    sends.start("leftb", "rightb")
    sends.wait_recv(*(f"{side}{k}" for side in ("right", "left") for k in range(3)))
    sends.wait_recv("downm", "upm", "leftt", "rightt", "leftb", "rightb")
    sends.wait_send()


def halo(objects, phase, pick, pick_t):
    tile = objects.shape[1]
    size = tile + 2 * HALF
    vmem = pl.BlockSpec(memory_space=pltpu.VMEM)
    return pl.pallas_call(
        halo_kernel,
        out_shape=(
            pltpu.VMEM((4, size, size), jnp.bfloat16),
            pltpu.VMEM((2, EXTENT, EXTENT), jnp.float32),
            pltpu.VMEM((4, size, size), jnp.float32),
        ),
        in_specs=[pl.BlockSpec(memory_space=pltpu.HBM)] * 4,
        out_specs=(vmem, vmem, vmem),
        scratch_shapes=[
            pltpu.VMEM(objects.shape, jnp.float32),
            pltpu.VMEM((EXTENT, EXTENT), jnp.float32),
            pltpu.VMEM((2, EXTENT, EXTENT), jnp.bfloat16),
            pltpu.SemaphoreType.DMA((6,)),
            pltpu.SemaphoreType.DMA((16,)),
            pltpu.SemaphoreType.DMA((16,)),
        ],
        compiler_params=pltpu.CompilerParams(
            collective_id=0, has_side_effects=True, vmem_limit_bytes=24 * 2**20
        ),
    )(*(pltpu.with_memory_space_constraint(x, pltpu.HBM) for x in (objects, phase, pick, pick_t)))


def margin_kernel(
    acc, out, row_send, row_recv, col_send, col_recv, corner_send, corner_recv, send, recv
):
    tile = out.shape[1]
    near, far, end = HALF, HALF + tile, 2 * HALF + tile
    own = slice(near, far)
    edges = (slice(0, near), slice(far, end))
    inner = slice(near, tile - near)
    outer = (slice(0, near), slice(tile - near, tile))
    place = Place()
    place.greet()
    rows = ((place.has_above, place.above), (place.has_below, place.below))
    cols = ((place.has_left, place.left), (place.has_right, place.right))

    sends = Sends(send, recv)
    for side, (there, device) in enumerate(cols):
        back = cols[1 - side][0]
        sends.add(f"corner{side}", corner_send.at[side], corner_recv.at[1 - side], device, there, back)
        sends.add(f"col{side}", col_send.at[side], col_recv.at[1 - side], device, there, back)
    for side, (there, device) in enumerate(rows):
        back = rows[1 - side][0]
        for name, part in (("m", inner), ("l", outer[0]), ("r", outer[1])):
            sends.add(
                f"row{side}{name}", row_send.at[side, :, :, part], row_recv.at[1 - side, :, :, part],
                device, there, back,
            )

    for c in range(2):
        for r in range(2):
            corner_send[c, r] = acc[:, edges[r], edges[c]].astype(jnp.bfloat16)
        sends.start(f"corner{c}")
    for r in range(2):
        row_send[r, :, :, inner] = acc[:, edges[r], 2 * near:tile].astype(jnp.bfloat16)
        sends.start(f"row{r}m")
    for c in range(2):
        for plane in range(4):
            col_send[c, plane] = acc[plane, own, edges[c]].astype(jnp.bfloat16)
        sends.start(f"col{c}")

    for side in range(2):
        @pl.when(jnp.logical_not(cols[side][0]))
        def _(side=side):
            corner_recv[side] = jnp.zeros(corner_recv.shape[1:], jnp.bfloat16)
            col_recv[side] = jnp.zeros(col_recv.shape[1:], jnp.bfloat16)

        @pl.when(jnp.logical_not(rows[side][0]))
        def _(side=side):
            row_recv[side] = jnp.zeros(row_recv.shape[1:], jnp.bfloat16)

    sends.wait_recv("corner0", "corner1")
    for r in range(2):
        for c, name in enumerate("lr"):
            at = slice(near + outer[c].start, near + outer[c].stop)
            total = acc[:, edges[r], at] + corner_recv[c, r].astype(jnp.float32)
            row_send[r, :, :, outer[c]] = total.astype(jnp.bfloat16)
            sends.start(f"row{r}{name}")

    for plane in range(4):
        out[plane] = acc[plane, own, own]
    sends.wait_recv("col0", "col1")
    for c in range(2):
        for plane in range(4):
            out[plane, :, outer[c]] += col_recv[c, plane].astype(jnp.float32)
    sends.wait_recv("row0m", "row1m", "row0l", "row1l", "row0r", "row1r")
    for r in range(2):
        for plane in range(4):
            out[plane, outer[r], :] += row_recv[r, plane].astype(jnp.float32)
    sends.wait_send()


def margins(acc, tile):
    vmem = pl.BlockSpec(memory_space=pltpu.VMEM)
    row = pltpu.VMEM((2, 4, HALF, tile), jnp.bfloat16)
    col = pltpu.VMEM((2, 4, tile, HALF), jnp.bfloat16)
    corner = pltpu.VMEM((2, 2, 4, HALF, HALF), jnp.bfloat16)
    return pl.pallas_call(
        margin_kernel,
        out_shape=pltpu.VMEM((4, tile, tile), jnp.float32),
        in_specs=[vmem],
        out_specs=vmem,
        scratch_shapes=[
            row, row, col, col, corner, corner,
            pltpu.SemaphoreType.DMA((10,)),
            pltpu.SemaphoreType.DMA((10,)),
        ],
        compiler_params=pltpu.CompilerParams(
            collective_id=1, has_side_effects=True, vmem_limit_bytes=32 * 2**20
        ),
    )(acc)


def output_fold(a, b, first):
    (ca, sa), (cb, sb) = a, b
    if first is None:
        return (ca + sb, cb - sa), (ca - sb, cb + sa)
    sa0, sb0 = jnp.where(first, 0.0, sa), jnp.where(first, 0.0, sb)
    low, high = jnp.where(first, sa, ca), jnp.where(first, sb, cb)
    return (ca + sb0, cb - sa0), (low - sb0, high + sa0)


def input_fold(top, bottom, first):
    (tr, ti), (br, bi) = top, bottom
    if first is None:
        return (tr + br, bi - ti), (ti + bi, tr - br)
    br0, bi0 = jnp.where(first, 0.0, br), jnp.where(first, 0.0, bi)
    return (tr + br0, jnp.where(first, br, bi - ti)), (ti + bi0, jnp.where(first, bi, tr - br))


def times(a, b):
    return a[0] * b[0] - a[1] * b[1], a[0] * b[1] + a[1] * b[0]


def conj_times(a, b):
    return a[0] * b[0] + a[1] * b[1], a[0] * b[1] - a[1] * b[0]


ROWS = 32
FULL = tuple(slice(r, r + ROWS) for r in range(0, EXTENT, ROWS))
UPPER = FULL[: len(FULL) // 2]
LEFT, RIGHT = slice(0, HALF), slice(HALF, EXTENT)


def one_slot(k, live, row, col, light, spread, table, table_t, pick, pick_t, ext, acc, measured,
             field, upper, folded, passed, ordered):
    cols = pl.ds(pl.multiple_of(col * HALF, HALF), EXTENT)
    lane = lax.broadcasted_iota(jnp.int32, (ROWS, HALF), 1) == 0
    top_row = lax.broadcasted_iota(jnp.int32, (ROWS, EXTENT), 0) == 0

    def place(rows):
        return pl.ds(pl.multiple_of(row * HALF + rows.start, ROWS), ROWS)

    def patch(plane, rows):
        at = place(rows)
        return tuple(ext[plane + i, at, cols].astype(jnp.float32) for i in range(2))

    def pair(ref, rows):
        return ref[0, rows, :], ref[1, rows, :]

    def put(ref, rows, value, columns=slice(None)):
        ref[0, rows, columns] = half(value[0])
        ref[1, rows, columns] = half(value[1])

    def add(plane, rows, value):
        at = place(rows)
        for i in range(2):
            acc[plane + i, at, cols] += value[i]

    def wave():
        for rows in FULL:
            put(field, rows, times(pair(light, rows), patch(0, rows)))
        ordered[...] = half(product(pick[...], measured[...]))

    def across():
        a, b = product(field[0], table[...]), product(field[1], table[...])
        for rows in FULL:
            low, high = output_fold(
                (a[rows, LEFT], a[rows, RIGHT]), (b[rows, LEFT], b[rows, RIGHT]), lane
            )
            put(upper, rows, low, LEFT)
            put(upper, rows, high, RIGHT)

    def frequency(act):
        def run():
            a, b = product(table_t[...], upper[0]), product(table_t[...], upper[1])
            for rows in UPPER:
                lower = slice(rows.start + HALF, rows.stop + HALF)
                first = top_row if rows.start == 0 else None
                low, high = output_fold((a[rows], a[lower]), (b[rows], b[lower]), first)
                x, y = input_fold(act(low, rows), act(high, lower), first)
                folded[0, rows, :], folded[0, lower, :] = half(x[0]), half(x[1])
                folded[1, rows, :], folded[1, lower, :] = half(y[0]), half(y[1])
        return run

    def down():
        a, b = product(table[...], folded[0]), product(table[...], folded[1])
        for rows in FULL:
            x, y = input_fold(
                (a[rows, LEFT], b[rows, LEFT]), (a[rows, RIGHT], b[rows, RIGHT]), lane
            )
            upper[0, rows, LEFT], upper[0, rows, RIGHT] = half(x[0]), half(x[1])
            upper[1, rows, LEFT], upper[1, rows, RIGHT] = half(y[0]), half(y[1])

    def space(act):
        def run():
            a, b = product(upper[0], table_t[...]), product(upper[1], table_t[...])
            for rows in FULL:
                act((a[rows], b[rows]), rows)
        return run

    def mix(value, rows):
        return times(pair(spread, rows), value)

    def revert(value, rows):
        return conj_times(pair(spread, rows), value)

    def second(value, rows):
        passed[0, rows, :], passed[1, rows, :] = value
        put(field, rows, times(value, patch(2, rows)))

    def pull():
        intensity = product(ordered[...], pick_t[...])

        def act(value, rows):
            misfit = value[0] * value[0] + value[1] * value[1] - intensity[rows]
            if live is not None:
                misfit = misfit * live
            return misfit * value[0], misfit * value[1]

        frequency(act)()

    def inward(value, rows):
        put(field, rows, conj_times(patch(2, rows), value))
        add(2, rows, conj_times(pair(passed, rows), value))

    def first(value, rows):
        add(0, rows, conj_times(pair(light, rows), value))

    return (
        wave, across, frequency(mix), down, space(second),
        across, pull, down, space(inward),
        across, frequency(revert), down, space(first),
    )


def slot_kernel(
    offsets, count, intensity, light, spread, table, table_t, pick, pick_t, ext, blank, acc,
    measured, field, upper, folded, passed, ordered, sems,
):
    number = count[0]
    steps = lax.div(number + 1, 2)

    def fetch(i, buf):
        return pltpu.make_async_copy(
            intensity.at[pl.ds(2 * i, 2)], measured.at[buf], sems.at[buf]
        )

    @pl.when(steps > 0)
    def _():
        fetch(0, 0).start()

    def one(i, carry):
        buf = lax.rem(i, 2)
        fetch(i, buf).wait()

        @pl.when(i + 1 < steps)
        def _():
            fetch(i + 1, 1 - buf).start()

        live = (2 * i + 1 < number).astype(jnp.float32)
        stages = [
            one_slot(
                k, live if k else None, offsets[0, 2 * i + k] + 1, offsets[1, 2 * i + k] + 1,
                light, spread, table, table_t, pick, pick_t, ext, acc, measured.at[buf, k],
                field.at[k], upper.at[k], folded.at[k], passed.at[k], ordered.at[k],
            )
            for k in range(2)
        ]
        for together in zip(*stages):
            for stage in together:
                stage()
        return carry

    lax.fori_loop(0, steps, one, 0)


def run_slots(offsets, count, intensity, light, spread, constants, ext, acc):
    smem = pl.BlockSpec(memory_space=pltpu.SMEM)
    vmem = pl.BlockSpec(memory_space=pltpu.VMEM)
    return pl.pallas_call(
        slot_kernel,
        out_shape=pltpu.VMEM(ext.shape, jnp.float32),
        in_specs=[smem, smem, pl.BlockSpec(memory_space=pltpu.HBM)] + [vmem] * 8,
        out_specs=vmem,
        scratch_shapes=[
            pltpu.VMEM((2, 2, EXTENT, EXTENT), jnp.bfloat16),
            pltpu.VMEM((2, 2, EXTENT, EXTENT), jnp.bfloat16),
            pltpu.VMEM((2, 2, EXTENT, EXTENT), jnp.bfloat16),
            pltpu.VMEM((2, 2, EXTENT, EXTENT), jnp.bfloat16),
            pltpu.VMEM((2, 2, EXTENT, EXTENT), jnp.float32),
            pltpu.VMEM((2, EXTENT, EXTENT), jnp.bfloat16),
            pltpu.SemaphoreType.DMA((2,)),
        ],
        input_output_aliases={10: 0},
        compiler_params=pltpu.CompilerParams(vmem_limit_bytes=16 * 2**20),
        cost_estimate=pl.CostEstimate(flops=12 * 26 * 2**25, bytes_accessed=2**24, transcendentals=0),
    )(offsets, count, intensity, light, spread, *constants, ext, acc)


def per_device(objects, illumination, propagator_phase, intensity, offsets, counts):
    constants = tables(EXTENT)
    ext, spread, acc = halo(objects, propagator_phase, *constants[2:])
    acc = run_slots(offsets.T, counts, intensity, illumination, spread, constants, ext, acc)
    return margins(acc, objects.shape[1])


def solution(mesh):
    placed = (
        P(None, "row", "col"),
        P(),
        P(),
        P(("row", "col"), None, None),
        P(("row", "col"), None),
        P(("row", "col")),
    )
    return jax.shard_map(
        per_device, mesh=mesh, in_specs=placed, out_specs=P(None, "row", "col"), check_vma=False
    )
```

```python
import math

import jax
import jax.numpy as jnp
import numpy as np
from jax import lax
from jax.experimental import pallas as pl
from jax.experimental.pallas import tpu as pltpu
from jax.sharding import PartitionSpec as P

EXTENT = 256
HALF = EXTENT // 2
MESH = pl.DeviceIdType.MESH


def tables(extent):
    half = extent // 2
    number = np.arange(extent, dtype=np.int32)
    turns = number[:, None] * number[None, :] % extent
    angle = turns.astype(np.float32) * np.float32(2.0 * math.pi / extent)
    scale = np.float32(1.0 / math.sqrt(extent))
    cosine = (np.cos(angle) * scale).astype(jnp.bfloat16)
    sine = (np.sin(angle) * scale).astype(jnp.bfloat16)
    folded = np.concatenate([cosine[:, : half + 1], sine[:, 1:half]], axis=1)
    order = np.concatenate([number[: half + 1], extent - number[1:half]])
    pick = np.eye(extent, dtype=np.float32)[order].astype(jnp.bfloat16)
    return tuple(jnp.asarray(np.ascontiguousarray(x)) for x in (folded, folded.T, pick, pick.T))


def product(a, b):
    return jnp.dot(a, b, preferred_element_type=jnp.float32)


def half(x):
    return x.astype(jnp.bfloat16)


SEAM = (7, 8)
RELAYS = ((3, 10), (5, 12))
PARTNERS = {7: (3, 5), 8: (10, 12), 3: (7, 10), 5: (7, 12), 10: (8, 3), 12: (8, 5)}


class Place:
    def __init__(self):
        r, c = lax.axis_index("row"), lax.axis_index("col")
        self.r, self.c = r, c
        self.has_above, self.has_below = r > 0, r < lax.axis_size("row") - 1
        self.has_left, self.has_right = c > 0, c < lax.axis_size("col") - 1
        self.above, self.below = (r - 1, c), (r + 1, c)
        self.left, self.right = (r, c - 1), (r, c + 1)
        self.sides = (
            (self.has_above, self.above),
            (self.has_below, self.below),
            (self.has_left, self.left),
            (self.has_right, self.right),
        )

    def greet(self):
        barrier = pltpu.get_barrier_semaphore()
        for there, device in self.sides:
            @pl.when(there)
            def _(device=device):
                pl.semaphore_signal(barrier, inc=1, device_id=device, device_id_type=MESH)

        for column, partners in PARTNERS.items():
            @pl.when(self.c == column)
            def _(partners=partners):
                for other in partners:
                    pl.semaphore_signal(barrier, inc=1, device_id=(self.r, other), device_id_type=MESH)

        count = sum(there.astype(jnp.int32) for there, _ in self.sides)
        count = count + 2 * sum((self.c == column).astype(jnp.int32) for column in PARTNERS)
        pl.semaphore_wait(barrier, count)


class Sends:
    def __init__(self, send, recv):
        self.send, self.recv, self.all = send, recv, {}

    def add(self, key, source, target, device, sent, received):
        k = len(self.all)
        copy = pltpu.make_async_remote_copy(
            src_ref=source, dst_ref=target, send_sem=self.send.at[k], recv_sem=self.recv.at[k],
            device_id=device, device_id_type=MESH,
        )
        self.all[key] = (copy, sent, received)

    def start(self, *keys):
        for key in keys:
            copy, sent, _ = self.all[key]
            pl.when(sent)(copy.start)

    def wait_recv(self, *keys):
        for key in keys:
            copy, _, received = self.all[key]
            pl.when(received)(copy.wait_recv)

    def relay(self, place, sources, targets, near, far):
        for g, pair in enumerate(RELAYS):
            planes = pl.ds(2 * g, 2)
            for side in range(2):
                device = tuple((place.r, column) for column in (pair[side], pair[1 - side], SEAM[side]))
                here = tuple(place.c == column for column in (pair[side], pair[1 - side], SEAM[side]))
                self.add(f"seam1{g}{side}", sources[side](planes), near, device[0], here[2], here[0])
                self.add(f"seam2{g}{side}", near, far, device[1], here[0], here[1])
                self.add(f"seam3{g}{side}", far, targets[side](planes), device[2], here[0], here[2])

    def start_seam(self, step):
        self.start(*(f"seam{step}{g}{side}" for g in range(2) for side in range(2)))

    def wait_seam(self, step):
        self.wait_recv(*(f"seam{step}{g}{side}" for g in range(2) for side in range(2)))

    def wait_send(self):
        for copy, sent, _ in self.all.values():
            pl.when(sent)(copy.wait_send)


def both(a, b):
    return jnp.logical_and(a, b)


def halo_kernel(
    objects, phase, pick, pick_t, ext, spread, acc, stage, angle, order, near_relay, far_relay,
    loads, send, recv
):
    tile = objects.shape[1]
    near, far, end = HALF, HALF + tile, 2 * HALF + tile
    own = slice(near, far)
    first, last = slice(0, near), slice(far, end)
    top, bottom = slice(near, 2 * near), slice(tile, far)
    place = Place()
    bands = ((tile - HALF, HALF), (0, HALF), (HALF, tile - 2 * HALF))
    loading = [
        pltpu.make_async_copy(objects.at[:, pl.ds(at, size)], stage.at[:, pl.ds(at, size)], loads.at[k])
        for k, (at, size) in enumerate(bands)
    ]
    parameters = [
        pltpu.make_async_copy(source, target, loads.at[3 + k])
        for k, (source, target) in enumerate(
            ((phase, angle), (pick, order.at[0]), (pick_t, order.at[1]))
        )
    ]
    for copy in loading + parameters:
        copy.start()
    place.greet()

    sends = Sends(send, recv)

    def route(key, source, target, device, sent, received):
        sends.add(key, ext.at[(slice(None),) + source], ext.at[(slice(None),) + target], device, sent, received)

    middle = slice(2 * near, tile)
    every, early, late = slice(None), slice(0, 2), slice(2, 4)
    for name, planes, cols in (
        ("l", every, top), ("r", every, bottom), ("m", early, middle), ("n", late, middle)
    ):
        for way, source, target, device, sent, received in (
            ("down", bottom, first, place.below, place.has_below, place.has_above),
            ("up", top, last, place.above, place.has_above, place.has_below),
        ):
            sends.add(way + name, ext.at[planes, source, cols], ext.at[planes, target, cols],
                      device, sent, received)
    for k, (at, size) in enumerate(bands):
        rows = slice(near + at, near + at + size)
        at_left, at_right = place.c != SEAM[0], place.c != SEAM[1]
        route(f"right{k}", (rows, bottom), (rows, first), place.right,
              both(place.has_right, at_left), both(place.has_left, at_right))
        route(f"left{k}", (rows, top), (rows, last), place.left,
              both(place.has_left, at_right), both(place.has_right, at_left))
    sends.relay(
        place,
        (lambda p: ext.at[p, own, bottom], lambda p: ext.at[p, own, top]),
        (lambda p: ext.at[p, own, last], lambda p: ext.at[p, own, first]),
        near_relay, far_relay,
    )
    for name, rows, there in (("t", first, place.has_above), ("b", last, place.has_below)):
        route("right" + name, (rows, bottom), (rows, first), place.right,
              both(place.has_right, there), both(place.has_left, there))
        route("left" + name, (rows, top), (rows, last), place.left,
              both(place.has_left, there), both(place.has_right, there))

    def cast(k):
        loading[k].wait()
        at, size = bands[k]
        for plane in range(4):
            ext[plane, near + at:near + at + size, near:far] = stage[plane, at:at + size].astype(jnp.bfloat16)

    cast(0)
    sends.start("downl", "downr", "right0", "left0")
    cast(1)
    sends.start("upl", "upr", "right1", "left1")
    cast(2)
    sends.start("right2", "left2")
    sends.start_seam(1)
    sends.start("downm", "upm")

    def blank(there, rows, cols):
        @pl.when(jnp.logical_not(there))
        def _():
            part = ext.at[:, rows, cols]
            part[...] = jnp.zeros(part.shape, jnp.bfloat16)

    blank(place.has_above, first, own)
    blank(place.has_below, last, own)
    blank(place.has_left, own, first)
    blank(place.has_right, own, last)
    for rows, there in ((first, place.has_above), (last, place.has_below)):
        blank(both(there, place.has_left), rows, first)
        blank(both(there, place.has_right), rows, last)
    sends.wait_seam(1)
    sends.start_seam(2)
    sends.start("downn", "upn")
    for copy in parameters:
        copy.wait()
    rest, ordered = angle[...], 0.0
    for _ in range(3):
        part = half(rest)
        rest = rest - part.astype(jnp.float32)
        ordered = ordered + product(half(product(order[0], part)), order[1])
    spread[0] = jnp.cos(ordered)
    spread[1] = jnp.sin(ordered)
    for plane in range(4):
        acc[plane] = jnp.zeros(acc.shape[1:], jnp.float32)

    sends.wait_recv("downl", "downr")
    sends.start("leftt", "rightt")
    sends.wait_recv("upl", "upr")
    sends.start("leftb", "rightb")
    sends.wait_seam(2)
    sends.start_seam(3)
    sends.wait_recv(*(f"{side}{k}" for side in ("right", "left") for k in range(3)))
    sends.wait_seam(3)
    sends.wait_recv("downn", "upn", "downm", "upm", "leftt", "rightt", "leftb", "rightb")
    sends.wait_send()


def halo(objects, phase, pick, pick_t):
    tile = objects.shape[1]
    size = tile + 2 * HALF
    relay = pltpu.VMEM((2, tile, HALF), jnp.bfloat16)
    vmem = pl.BlockSpec(memory_space=pltpu.VMEM)
    return pl.pallas_call(
        halo_kernel,
        out_shape=(
            pltpu.VMEM((4, size, size), jnp.bfloat16),
            pltpu.VMEM((2, EXTENT, EXTENT), jnp.float32),
            pltpu.VMEM((4, size, size), jnp.float32),
        ),
        in_specs=[pl.BlockSpec(memory_space=pltpu.HBM)] * 4,
        out_specs=(vmem, vmem, vmem),
        scratch_shapes=[
            pltpu.VMEM(objects.shape, jnp.float32),
            pltpu.VMEM((EXTENT, EXTENT), jnp.float32),
            pltpu.VMEM((2, EXTENT, EXTENT), jnp.bfloat16),
            relay,
            relay,
            pltpu.SemaphoreType.DMA((6,)),
            pltpu.SemaphoreType.DMA((30,)),
            pltpu.SemaphoreType.DMA((30,)),
        ],
        compiler_params=pltpu.CompilerParams(
            collective_id=0, has_side_effects=True, vmem_limit_bytes=24 * 2**20
        ),
    )(*(pltpu.with_memory_space_constraint(x, pltpu.HBM) for x in (objects, phase, pick, pick_t)))


def margin_kernel(
    acc, out, row_send, row_recv, col_send, col_recv, corner_send, corner_recv,
    near_relay, far_relay, send, recv
):
    tile = out.shape[1]
    near, far, end = HALF, HALF + tile, 2 * HALF + tile
    own = slice(near, far)
    edges = (slice(0, near), slice(far, end))
    inner = slice(near, tile - near)
    outer = (slice(0, near), slice(tile - near, tile))
    place = Place()
    place.greet()
    rows = ((place.has_above, place.above), (place.has_below, place.below))
    cols = ((place.has_left, place.left), (place.has_right, place.right))

    sends = Sends(send, recv)
    for side, (there, device) in enumerate(cols):
        back = cols[1 - side][0]
        sends.add(f"corner{side}", corner_send.at[side], corner_recv.at[1 - side], device, there, back)
        sends.add(f"col{side}", col_send.at[side], col_recv.at[1 - side], device,
                  both(there, place.c != SEAM[1 - side]), both(back, place.c != SEAM[side]))
    sends.relay(
        place,
        (lambda p: col_send.at[1, p], lambda p: col_send.at[0, p]),
        (lambda p: col_recv.at[1, p], lambda p: col_recv.at[0, p]),
        near_relay, far_relay,
    )
    for side, (there, device) in enumerate(rows):
        back = rows[1 - side][0]
        for name, part in (("m", inner), ("l", outer[0]), ("r", outer[1])):
            sends.add(
                f"row{side}{name}", row_send.at[side, :, :, part], row_recv.at[1 - side, :, :, part],
                device, there, back,
            )

    for c in range(2):
        for r in range(2):
            corner_send[c, r] = acc[:, edges[r], edges[c]].astype(jnp.bfloat16)
        sends.start(f"corner{c}")
    for r in range(2):
        row_send[r, :, :, inner] = acc[:, edges[r], 2 * near:tile].astype(jnp.bfloat16)
        sends.start(f"row{r}m")
    for c in range(2):
        for plane in range(4):
            col_send[c, plane] = acc[plane, own, edges[c]].astype(jnp.bfloat16)
        sends.start(f"col{c}")
    sends.start_seam(1)

    for side in range(2):
        @pl.when(jnp.logical_not(cols[side][0]))
        def _(side=side):
            corner_recv[side] = jnp.zeros(corner_recv.shape[1:], jnp.bfloat16)
            col_recv[side] = jnp.zeros(col_recv.shape[1:], jnp.bfloat16)

        @pl.when(jnp.logical_not(rows[side][0]))
        def _(side=side):
            row_recv[side] = jnp.zeros(row_recv.shape[1:], jnp.bfloat16)

    sends.wait_seam(1)
    sends.start_seam(2)
    sends.wait_recv("corner0", "corner1")
    for r in range(2):
        for c, name in enumerate("lr"):
            at = slice(near + outer[c].start, near + outer[c].stop)
            total = acc[:, edges[r], at] + corner_recv[c, r].astype(jnp.float32)
            row_send[r, :, :, outer[c]] = total.astype(jnp.bfloat16)
            sends.start(f"row{r}{name}")

    for plane in range(4):
        out[plane] = acc[plane, own, own]
    sends.wait_seam(2)
    sends.start_seam(3)
    sends.wait_recv("col0", "col1")
    sends.wait_seam(3)
    for c in range(2):
        for plane in range(4):
            out[plane, :, outer[c]] += col_recv[c, plane].astype(jnp.float32)
    sends.wait_recv("row0m", "row1m", "row0l", "row1l", "row0r", "row1r")
    for r in range(2):
        for plane in range(4):
            out[plane, outer[r], :] += row_recv[r, plane].astype(jnp.float32)
    sends.wait_send()


def margins(acc, tile):
    vmem = pl.BlockSpec(memory_space=pltpu.VMEM)
    row = pltpu.VMEM((2, 4, HALF, tile), jnp.bfloat16)
    col = pltpu.VMEM((2, 4, tile, HALF), jnp.bfloat16)
    relay = pltpu.VMEM((2, tile, HALF), jnp.bfloat16)
    corner = pltpu.VMEM((2, 2, 4, HALF, HALF), jnp.bfloat16)
    return pl.pallas_call(
        margin_kernel,
        out_shape=pltpu.VMEM((4, tile, tile), jnp.float32),
        in_specs=[vmem],
        out_specs=vmem,
        scratch_shapes=[
            row, row, col, col, corner, corner, relay, relay,
            pltpu.SemaphoreType.DMA((22,)),
            pltpu.SemaphoreType.DMA((22,)),
        ],
        compiler_params=pltpu.CompilerParams(
            collective_id=1, has_side_effects=True, vmem_limit_bytes=32 * 2**20
        ),
    )(acc)


def output_fold(a, b, first):
    (ca, sa), (cb, sb) = a, b
    if first is None:
        return (ca + sb, cb - sa), (ca - sb, cb + sa)
    sa0, sb0 = jnp.where(first, 0.0, sa), jnp.where(first, 0.0, sb)
    low, high = jnp.where(first, sa, ca), jnp.where(first, sb, cb)
    return (ca + sb0, cb - sa0), (low - sb0, high + sa0)


def input_fold(top, bottom, first):
    (tr, ti), (br, bi) = top, bottom
    if first is None:
        return (tr + br, bi - ti), (ti + bi, tr - br)
    br0, bi0 = jnp.where(first, 0.0, br), jnp.where(first, 0.0, bi)
    return (tr + br0, jnp.where(first, br, bi - ti)), (ti + bi0, jnp.where(first, bi, tr - br))


def times(a, b):
    return a[0] * b[0] - a[1] * b[1], a[0] * b[1] + a[1] * b[0]


def conj_times(a, b):
    return a[0] * b[0] + a[1] * b[1], a[0] * b[1] - a[1] * b[0]


ROWS = 32
FULL = tuple(slice(r, r + ROWS) for r in range(0, EXTENT, ROWS))
UPPER = FULL[: len(FULL) // 2]
LEFT, RIGHT = slice(0, HALF), slice(HALF, EXTENT)


def one_slot(k, live, row, col, light, spread, table, table_t, pick, pick_t, ext, acc, measured,
             field, upper, folded, passed, ordered):
    cols = pl.ds(pl.multiple_of(col * HALF, HALF), EXTENT)
    lane = lax.broadcasted_iota(jnp.int32, (ROWS, HALF), 1) == 0
    top_row = lax.broadcasted_iota(jnp.int32, (ROWS, EXTENT), 0) == 0

    def place(rows):
        return pl.ds(pl.multiple_of(row * HALF + rows.start, ROWS), ROWS)

    def patch(plane, rows):
        at = place(rows)
        return tuple(ext[plane + i, at, cols].astype(jnp.float32) for i in range(2))

    def pair(ref, rows):
        return ref[0, rows, :], ref[1, rows, :]

    def put(ref, rows, value, columns=slice(None)):
        ref[0, rows, columns] = half(value[0])
        ref[1, rows, columns] = half(value[1])

    def add(plane, rows, value):
        at = place(rows)
        for i in range(2):
            acc[plane + i, at, cols] += value[i]

    def wave():
        for rows in FULL:
            put(field, rows, times(pair(light, rows), patch(0, rows)))
        ordered[...] = half(product(pick[...], measured[...]))

    def across():
        a, b = product(field[0], table[...]), product(field[1], table[...])
        for rows in FULL:
            low, high = output_fold(
                (a[rows, LEFT], a[rows, RIGHT]), (b[rows, LEFT], b[rows, RIGHT]), lane
            )
            put(upper, rows, low, LEFT)
            put(upper, rows, high, RIGHT)

    def frequency(act):
        def run():
            a, b = product(table_t[...], upper[0]), product(table_t[...], upper[1])
            for rows in UPPER:
                lower = slice(rows.start + HALF, rows.stop + HALF)
                first = top_row if rows.start == 0 else None
                low, high = output_fold((a[rows], a[lower]), (b[rows], b[lower]), first)
                x, y = input_fold(act(low, rows), act(high, lower), first)
                folded[0, rows, :], folded[0, lower, :] = half(x[0]), half(x[1])
                folded[1, rows, :], folded[1, lower, :] = half(y[0]), half(y[1])
        return run

    def down():
        a, b = product(table[...], folded[0]), product(table[...], folded[1])
        for rows in FULL:
            x, y = input_fold(
                (a[rows, LEFT], b[rows, LEFT]), (a[rows, RIGHT], b[rows, RIGHT]), lane
            )
            upper[0, rows, LEFT], upper[0, rows, RIGHT] = half(x[0]), half(x[1])
            upper[1, rows, LEFT], upper[1, rows, RIGHT] = half(y[0]), half(y[1])

    def space(act):
        def run():
            a, b = product(upper[0], table_t[...]), product(upper[1], table_t[...])
            for rows in FULL:
                act((a[rows], b[rows]), rows)
        return run

    def mix(value, rows):
        return times(pair(spread, rows), value)

    def revert(value, rows):
        return conj_times(pair(spread, rows), value)

    def second(value, rows):
        passed[0, rows, :], passed[1, rows, :] = value
        put(field, rows, times(value, patch(2, rows)))

    def pull():
        intensity = product(ordered[...], pick_t[...])

        def act(value, rows):
            misfit = value[0] * value[0] + value[1] * value[1] - intensity[rows]
            if live is not None:
                misfit = misfit * live
            return misfit * value[0], misfit * value[1]

        frequency(act)()

    def inward(value, rows):
        put(field, rows, conj_times(patch(2, rows), value))
        add(2, rows, conj_times(pair(passed, rows), value))

    def first(value, rows):
        add(0, rows, conj_times(pair(light, rows), value))

    return (
        wave, across, frequency(mix), down, space(second),
        across, pull, down, space(inward),
        across, frequency(revert), down, space(first),
    )


def slot_kernel(
    offsets, count, intensity, light, spread, table, table_t, pick, pick_t, ext, blank, acc,
    measured, field, upper, folded, passed, ordered, sems,
):
    number = count[0]
    steps = lax.div(number + 1, 2)

    def fetch(i, buf):
        return pltpu.make_async_copy(
            intensity.at[pl.ds(2 * i, 2)], measured.at[buf], sems.at[buf]
        )

    @pl.when(steps > 0)
    def _():
        fetch(0, 0).start()

    def one(i, carry):
        buf = lax.rem(i, 2)
        fetch(i, buf).wait()

        @pl.when(i + 1 < steps)
        def _():
            fetch(i + 1, 1 - buf).start()

        live = (2 * i + 1 < number).astype(jnp.float32)
        stages = [
            one_slot(
                k, live if k else None, offsets[0, 2 * i + k] + 1, offsets[1, 2 * i + k] + 1,
                light, spread, table, table_t, pick, pick_t, ext, acc, measured.at[buf, k],
                field.at[k], upper.at[k], folded.at[k], passed.at[k], ordered.at[k],
            )
            for k in range(2)
        ]
        for together in zip(*stages):
            for stage in together:
                stage()
        return carry

    lax.fori_loop(0, steps, one, 0)


def run_slots(offsets, count, intensity, light, spread, constants, ext, acc):
    smem = pl.BlockSpec(memory_space=pltpu.SMEM)
    vmem = pl.BlockSpec(memory_space=pltpu.VMEM)
    return pl.pallas_call(
        slot_kernel,
        out_shape=pltpu.VMEM(ext.shape, jnp.float32),
        in_specs=[smem, smem, pl.BlockSpec(memory_space=pltpu.HBM)] + [vmem] * 8,
        out_specs=vmem,
        scratch_shapes=[
            pltpu.VMEM((2, 2, EXTENT, EXTENT), jnp.bfloat16),
            pltpu.VMEM((2, 2, EXTENT, EXTENT), jnp.bfloat16),
            pltpu.VMEM((2, 2, EXTENT, EXTENT), jnp.bfloat16),
            pltpu.VMEM((2, 2, EXTENT, EXTENT), jnp.bfloat16),
            pltpu.VMEM((2, 2, EXTENT, EXTENT), jnp.float32),
            pltpu.VMEM((2, EXTENT, EXTENT), jnp.bfloat16),
            pltpu.SemaphoreType.DMA((2,)),
        ],
        input_output_aliases={10: 0},
        compiler_params=pltpu.CompilerParams(vmem_limit_bytes=16 * 2**20),
        cost_estimate=pl.CostEstimate(flops=12 * 26 * 2**25, bytes_accessed=2**24, transcendentals=0),
    )(offsets, count, intensity, light, spread, *constants, ext, acc)


def per_device(objects, illumination, propagator_phase, intensity, offsets, counts):
    constants = tables(EXTENT)
    ext, spread, acc = halo(objects, propagator_phase, *constants[2:])
    acc = run_slots(offsets.T, counts, intensity, illumination, spread, constants, ext, acc)
    return margins(acc, objects.shape[1])


def solution(mesh):
    placed = (
        P(None, "row", "col"),
        P(),
        P(),
        P(("row", "col"), None, None),
        P(("row", "col"), None),
        P(("row", "col")),
    )
    return jax.shard_map(
        per_device, mesh=mesh, in_specs=placed, out_specs=P(None, "row", "col"), check_vma=False
    )
```

```python
import math

import jax
import jax.numpy as jnp
import numpy as np
from jax import lax
from jax.experimental import pallas as pl
from jax.experimental.pallas import tpu as pltpu
from jax.sharding import PartitionSpec as P

EXTENT = 256
HALF = EXTENT // 2
MESH = pl.DeviceIdType.MESH


def tables(extent):
    half = extent // 2
    number = np.arange(extent, dtype=np.int32)
    turns = number[:, None] * number[None, :] % extent
    angle = turns.astype(np.float32) * np.float32(2.0 * math.pi / extent)
    scale = np.float32(1.0 / math.sqrt(extent))
    cosine = (np.cos(angle) * scale).astype(jnp.bfloat16)
    sine = (np.sin(angle) * scale).astype(jnp.bfloat16)
    folded = np.concatenate([cosine[:, : half + 1], sine[:, 1:half]], axis=1)
    order = np.concatenate([number[: half + 1], extent - number[1:half]])
    pick = np.eye(extent, dtype=np.float32)[order].astype(jnp.bfloat16)
    return tuple(jnp.asarray(np.ascontiguousarray(x)) for x in (folded, folded.T, pick, pick.T))


def product(a, b):
    return jnp.dot(a, b, preferred_element_type=jnp.float32)


def half(x):
    return x.astype(jnp.bfloat16)


SEAM = (7, 8)
RELAYS = ((3, 10), (5, 12))
PARTNERS = {7: (3, 5), 8: (10, 12), 3: (7, 10), 5: (7, 12), 10: (8, 3), 12: (8, 5)}


class Place:
    def __init__(self):
        r, c = lax.axis_index("row"), lax.axis_index("col")
        self.r, self.c = r, c
        self.has_above, self.has_below = r > 0, r < lax.axis_size("row") - 1
        self.has_left, self.has_right = c > 0, c < lax.axis_size("col") - 1
        self.above, self.below = (r - 1, c), (r + 1, c)
        self.left, self.right = (r, c - 1), (r, c + 1)
        self.sides = (
            (self.has_above, self.above),
            (self.has_below, self.below),
            (self.has_left, self.left),
            (self.has_right, self.right),
        )

    def greet(self):
        barrier = pltpu.get_barrier_semaphore()
        for there, device in self.sides:
            @pl.when(there)
            def _(device=device):
                pl.semaphore_signal(barrier, inc=1, device_id=device, device_id_type=MESH)

        for column, partners in PARTNERS.items():
            @pl.when(self.c == column)
            def _(partners=partners):
                for other in partners:
                    pl.semaphore_signal(barrier, inc=1, device_id=(self.r, other), device_id_type=MESH)

        count = sum(there.astype(jnp.int32) for there, _ in self.sides)
        count = count + 2 * sum((self.c == column).astype(jnp.int32) for column in PARTNERS)
        pl.semaphore_wait(barrier, count)


class Sends:
    def __init__(self, send, recv):
        self.send, self.recv, self.all = send, recv, {}

    def add(self, key, source, target, device, sent, received):
        k = len(self.all)
        copy = pltpu.make_async_remote_copy(
            src_ref=source, dst_ref=target, send_sem=self.send.at[k], recv_sem=self.recv.at[k],
            device_id=device, device_id_type=MESH,
        )
        self.all[key] = (copy, sent, received)

    def start(self, *keys):
        for key in keys:
            copy, sent, _ = self.all[key]
            pl.when(sent)(copy.start)

    def wait_recv(self, *keys):
        for key in keys:
            copy, _, received = self.all[key]
            pl.when(received)(copy.wait_recv)

    def relay(self, place, sources, targets, near, far):
        for g, pair in enumerate(RELAYS):
            planes = pl.ds(2 * g, 2)
            for side in range(2):
                device = tuple((place.r, column) for column in (pair[side], pair[1 - side], SEAM[side]))
                here = tuple(place.c == column for column in (pair[side], pair[1 - side], SEAM[side]))
                self.add(f"seam1{g}{side}", sources[side](planes), near, device[0], here[2], here[0])
                self.add(f"seam2{g}{side}", near, far, device[1], here[0], here[1])
                self.add(f"seam3{g}{side}", far, targets[side](planes), device[2], here[0], here[2])

    def start_seam(self, step):
        self.start(*(f"seam{step}{g}{side}" for g in range(2) for side in range(2)))

    def wait_seam(self, step):
        self.wait_recv(*(f"seam{step}{g}{side}" for g in range(2) for side in range(2)))

    def wait_send(self):
        for copy, sent, _ in self.all.values():
            pl.when(sent)(copy.wait_send)


def both(a, b):
    return jnp.logical_and(a, b)


def halo_kernel(
    objects, phase, pick, pick_t, ext, spread, acc, stage, angle, order, near_relay, far_relay,
    loads, send, recv
):
    tile = objects.shape[1]
    near, far, end = HALF, HALF + tile, 2 * HALF + tile
    own = slice(near, far)
    first, last = slice(0, near), slice(far, end)
    top, bottom = slice(near, 2 * near), slice(tile, far)
    place = Place()
    bands = ((tile - HALF, HALF), (0, HALF), (HALF, tile - 2 * HALF))
    loading = [
        pltpu.make_async_copy(objects.at[:, pl.ds(at, size)], stage.at[:, pl.ds(at, size)], loads.at[k])
        for k, (at, size) in enumerate(bands)
    ]
    parameters = [
        pltpu.make_async_copy(source, target, loads.at[3 + k])
        for k, (source, target) in enumerate(
            ((phase, angle), (pick, order.at[0]), (pick_t, order.at[1]))
        )
    ]
    for copy in loading + parameters:
        copy.start()
    place.greet()

    sends = Sends(send, recv)

    def route(key, source, target, device, sent, received):
        sends.add(key, ext.at[(slice(None),) + source], ext.at[(slice(None),) + target], device, sent, received)

    middle = slice(2 * near, tile)
    every, early, late = slice(None), slice(0, 2), slice(2, 4)
    for name, planes, cols in (
        ("l", every, top), ("r", every, bottom), ("m", early, middle), ("n", late, middle)
    ):
        for way, source, target, device, sent, received in (
            ("down", bottom, first, place.below, place.has_below, place.has_above),
            ("up", top, last, place.above, place.has_above, place.has_below),
        ):
            sends.add(way + name, ext.at[planes, source, cols], ext.at[planes, target, cols],
                      device, sent, received)
    for k, (at, size) in enumerate(bands):
        rows = slice(near + at, near + at + size)
        at_left, at_right = place.c != SEAM[0], place.c != SEAM[1]
        route(f"right{k}", (rows, bottom), (rows, first), place.right,
              both(place.has_right, at_left), both(place.has_left, at_right))
        route(f"left{k}", (rows, top), (rows, last), place.left,
              both(place.has_left, at_right), both(place.has_right, at_left))
    sends.relay(
        place,
        (lambda p: ext.at[p, own, bottom], lambda p: ext.at[p, own, top]),
        (lambda p: ext.at[p, own, last], lambda p: ext.at[p, own, first]),
        near_relay, far_relay,
    )
    for name, rows, there in (("t", first, place.has_above), ("b", last, place.has_below)):
        route("right" + name, (rows, bottom), (rows, first), place.right,
              both(place.has_right, there), both(place.has_left, there))
        route("left" + name, (rows, top), (rows, last), place.left,
              both(place.has_left, there), both(place.has_right, there))

    def cast(k):
        loading[k].wait()
        at, size = bands[k]
        for plane in range(4):
            ext[plane, near + at:near + at + size, near:far] = stage[plane, at:at + size].astype(jnp.bfloat16)

    cast(0)
    sends.start("downl", "downr", "right0", "left0")
    cast(1)
    sends.start("upl", "upr", "right1", "left1")
    cast(2)
    sends.start("right2", "left2")
    sends.start_seam(1)
    sends.start("downm", "upm")

    def blank(there, rows, cols):
        @pl.when(jnp.logical_not(there))
        def _():
            part = ext.at[:, rows, cols]
            part[...] = jnp.zeros(part.shape, jnp.bfloat16)

    blank(place.has_above, first, own)
    blank(place.has_below, last, own)
    blank(place.has_left, own, first)
    blank(place.has_right, own, last)
    for rows, there in ((first, place.has_above), (last, place.has_below)):
        blank(both(there, place.has_left), rows, first)
        blank(both(there, place.has_right), rows, last)
    for copy in parameters:
        copy.wait()
    rest, ordered = angle[...], 0.0
    for _ in range(3):
        part = half(rest)
        rest = rest - part.astype(jnp.float32)
        ordered = ordered + product(half(product(order[0], part)), order[1])
    spread[0] = jnp.cos(ordered)
    spread[1] = jnp.sin(ordered)
    for plane in range(4):
        acc[plane] = jnp.zeros(acc.shape[1:], jnp.float32)

    sends.wait_seam(1)
    sends.start_seam(2)
    sends.wait_recv("downl", "downr")
    sends.start("leftt", "rightt")
    sends.wait_recv("upl", "upr")
    sends.start("leftb", "rightb")
    sends.start("downn", "upn")
    sends.wait_seam(2)
    sends.start_seam(3)
    sends.wait_recv(*(f"{side}{k}" for side in ("right", "left") for k in range(3)))
    sends.wait_seam(3)
    sends.wait_recv("downn", "upn", "downm", "upm", "leftt", "rightt", "leftb", "rightb")
    sends.wait_send()


def halo(objects, phase, pick, pick_t):
    tile = objects.shape[1]
    size = tile + 2 * HALF
    relay = pltpu.VMEM((2, tile, HALF), jnp.bfloat16)
    vmem = pl.BlockSpec(memory_space=pltpu.VMEM)
    return pl.pallas_call(
        halo_kernel,
        out_shape=(
            pltpu.VMEM((4, size, size), jnp.bfloat16),
            pltpu.VMEM((2, EXTENT, EXTENT), jnp.float32),
            pltpu.VMEM((4, size, size), jnp.float32),
        ),
        in_specs=[pl.BlockSpec(memory_space=pltpu.HBM)] * 4,
        out_specs=(vmem, vmem, vmem),
        scratch_shapes=[
            pltpu.VMEM(objects.shape, jnp.float32),
            pltpu.VMEM((EXTENT, EXTENT), jnp.float32),
            pltpu.VMEM((2, EXTENT, EXTENT), jnp.bfloat16),
            relay,
            relay,
            pltpu.SemaphoreType.DMA((6,)),
            pltpu.SemaphoreType.DMA((30,)),
            pltpu.SemaphoreType.DMA((30,)),
        ],
        compiler_params=pltpu.CompilerParams(
            collective_id=0, has_side_effects=True, vmem_limit_bytes=24 * 2**20
        ),
    )(*(pltpu.with_memory_space_constraint(x, pltpu.HBM) for x in (objects, phase, pick, pick_t)))


def margin_kernel(
    acc, out, row_send, row_recv, col_send, col_recv, corner_send, corner_recv,
    near_relay, far_relay, send, recv
):
    tile = out.shape[1]
    near, far, end = HALF, HALF + tile, 2 * HALF + tile
    own = slice(near, far)
    edges = (slice(0, near), slice(far, end))
    inner = slice(near, tile - near)
    outer = (slice(0, near), slice(tile - near, tile))
    place = Place()
    place.greet()
    rows = ((place.has_above, place.above), (place.has_below, place.below))
    cols = ((place.has_left, place.left), (place.has_right, place.right))

    sends = Sends(send, recv)
    for side, (there, device) in enumerate(cols):
        back = cols[1 - side][0]
        sends.add(f"corner{side}", corner_send.at[side], corner_recv.at[1 - side], device, there, back)
        sends.add(f"col{side}", col_send.at[side], col_recv.at[1 - side], device,
                  both(there, place.c != SEAM[1 - side]), both(back, place.c != SEAM[side]))
    sends.relay(
        place,
        (lambda p: col_send.at[1, p], lambda p: col_send.at[0, p]),
        (lambda p: col_recv.at[1, p], lambda p: col_recv.at[0, p]),
        near_relay, far_relay,
    )
    for side, (there, device) in enumerate(rows):
        back = rows[1 - side][0]
        for name, part in (("m", inner), ("l", outer[0]), ("r", outer[1])):
            sends.add(
                f"row{side}{name}", row_send.at[side, :, :, part], row_recv.at[1 - side, :, :, part],
                device, there, back,
            )

    for c in range(2):
        for r in range(2):
            corner_send[c, r] = acc[:, edges[r], edges[c]].astype(jnp.bfloat16)
        sends.start(f"corner{c}")
    for c in range(2):
        for plane in range(4):
            col_send[c, plane] = acc[plane, own, edges[c]].astype(jnp.bfloat16)
    sends.start_seam(1)
    for r in range(2):
        row_send[r, :, :, inner] = acc[:, edges[r], 2 * near:tile].astype(jnp.bfloat16)
        sends.start(f"row{r}m")
    sends.start("col0", "col1")

    for side in range(2):
        @pl.when(jnp.logical_not(cols[side][0]))
        def _(side=side):
            corner_recv[side] = jnp.zeros(corner_recv.shape[1:], jnp.bfloat16)
            col_recv[side] = jnp.zeros(col_recv.shape[1:], jnp.bfloat16)

        @pl.when(jnp.logical_not(rows[side][0]))
        def _(side=side):
            row_recv[side] = jnp.zeros(row_recv.shape[1:], jnp.bfloat16)

    sends.wait_recv("corner0", "corner1")
    for c, name in enumerate("lr"):
        if c == 1:
            sends.wait_seam(1)
            sends.start_seam(2)
        for r in range(2):
            at = slice(near + outer[c].start, near + outer[c].stop)
            total = acc[:, edges[r], at] + corner_recv[c, r].astype(jnp.float32)
            row_send[r, :, :, outer[c]] = total.astype(jnp.bfloat16)
            sends.start(f"row{r}{name}")

    for plane in range(4):
        out[plane] = acc[plane, own, own]
    sends.wait_seam(2)
    sends.start_seam(3)
    sends.wait_recv("col0", "col1")
    sends.wait_seam(3)
    for c in range(2):
        for plane in range(4):
            out[plane, :, outer[c]] += col_recv[c, plane].astype(jnp.float32)
    sends.wait_recv("row0m", "row1m", "row0l", "row1l", "row0r", "row1r")
    for r in range(2):
        for plane in range(4):
            out[plane, outer[r], :] += row_recv[r, plane].astype(jnp.float32)
    sends.wait_send()


def margins(acc, tile):
    vmem = pl.BlockSpec(memory_space=pltpu.VMEM)
    row = pltpu.VMEM((2, 4, HALF, tile), jnp.bfloat16)
    col = pltpu.VMEM((2, 4, tile, HALF), jnp.bfloat16)
    relay = pltpu.VMEM((2, tile, HALF), jnp.bfloat16)
    corner = pltpu.VMEM((2, 2, 4, HALF, HALF), jnp.bfloat16)
    return pl.pallas_call(
        margin_kernel,
        out_shape=pltpu.VMEM((4, tile, tile), jnp.float32),
        in_specs=[vmem],
        out_specs=vmem,
        scratch_shapes=[
            row, row, col, col, corner, corner, relay, relay,
            pltpu.SemaphoreType.DMA((22,)),
            pltpu.SemaphoreType.DMA((22,)),
        ],
        compiler_params=pltpu.CompilerParams(
            collective_id=1, has_side_effects=True, vmem_limit_bytes=32 * 2**20
        ),
    )(acc)


def output_fold(a, b, first):
    (ca, sa), (cb, sb) = a, b
    if first is None:
        return (ca + sb, cb - sa), (ca - sb, cb + sa)
    sa0, sb0 = jnp.where(first, 0.0, sa), jnp.where(first, 0.0, sb)
    low, high = jnp.where(first, sa, ca), jnp.where(first, sb, cb)
    return (ca + sb0, cb - sa0), (low - sb0, high + sa0)


def input_fold(top, bottom, first):
    (tr, ti), (br, bi) = top, bottom
    if first is None:
        return (tr + br, bi - ti), (ti + bi, tr - br)
    br0, bi0 = jnp.where(first, 0.0, br), jnp.where(first, 0.0, bi)
    return (tr + br0, jnp.where(first, br, bi - ti)), (ti + bi0, jnp.where(first, bi, tr - br))


def times(a, b):
    return a[0] * b[0] - a[1] * b[1], a[0] * b[1] + a[1] * b[0]


def conj_times(a, b):
    return a[0] * b[0] + a[1] * b[1], a[0] * b[1] - a[1] * b[0]


ROWS = 32
FULL = tuple(slice(r, r + ROWS) for r in range(0, EXTENT, ROWS))
UPPER = FULL[: len(FULL) // 2]
LEFT, RIGHT = slice(0, HALF), slice(HALF, EXTENT)


def one_slot(k, live, row, col, light, spread, table, table_t, pick, pick_t, ext, acc, measured,
             field, upper, folded, passed, ordered):
    cols = pl.ds(pl.multiple_of(col * HALF, HALF), EXTENT)
    lane = lax.broadcasted_iota(jnp.int32, (ROWS, HALF), 1) == 0
    top_row = lax.broadcasted_iota(jnp.int32, (ROWS, EXTENT), 0) == 0

    def place(rows):
        return pl.ds(pl.multiple_of(row * HALF + rows.start, ROWS), ROWS)

    def patch(plane, rows):
        at = place(rows)
        return tuple(ext[plane + i, at, cols].astype(jnp.float32) for i in range(2))

    def pair(ref, rows):
        return ref[0, rows, :], ref[1, rows, :]

    def put(ref, rows, value, columns=slice(None)):
        ref[0, rows, columns] = half(value[0])
        ref[1, rows, columns] = half(value[1])

    def add(plane, rows, value):
        at = place(rows)
        for i in range(2):
            acc[plane + i, at, cols] += value[i]

    def wave():
        for rows in FULL:
            put(field, rows, times(pair(light, rows), patch(0, rows)))
        ordered[...] = half(product(pick[...], measured[...]))

    def across():
        a, b = product(field[0], table[...]), product(field[1], table[...])
        for rows in FULL:
            low, high = output_fold(
                (a[rows, LEFT], a[rows, RIGHT]), (b[rows, LEFT], b[rows, RIGHT]), lane
            )
            put(upper, rows, low, LEFT)
            put(upper, rows, high, RIGHT)

    def frequency(act):
        def run():
            a, b = product(table_t[...], upper[0]), product(table_t[...], upper[1])
            for rows in UPPER:
                lower = slice(rows.start + HALF, rows.stop + HALF)
                first = top_row if rows.start == 0 else None
                low, high = output_fold((a[rows], a[lower]), (b[rows], b[lower]), first)
                x, y = input_fold(act(low, rows), act(high, lower), first)
                folded[0, rows, :], folded[0, lower, :] = half(x[0]), half(x[1])
                folded[1, rows, :], folded[1, lower, :] = half(y[0]), half(y[1])
        return run

    def down():
        a, b = product(table[...], folded[0]), product(table[...], folded[1])
        for rows in FULL:
            x, y = input_fold(
                (a[rows, LEFT], b[rows, LEFT]), (a[rows, RIGHT], b[rows, RIGHT]), lane
            )
            upper[0, rows, LEFT], upper[0, rows, RIGHT] = half(x[0]), half(x[1])
            upper[1, rows, LEFT], upper[1, rows, RIGHT] = half(y[0]), half(y[1])

    def space(act):
        def run():
            a, b = product(upper[0], table_t[...]), product(upper[1], table_t[...])
            for rows in FULL:
                act((a[rows], b[rows]), rows)
        return run

    def mix(value, rows):
        return times(pair(spread, rows), value)

    def revert(value, rows):
        return conj_times(pair(spread, rows), value)

    def second(value, rows):
        passed[0, rows, :], passed[1, rows, :] = value
        put(field, rows, times(value, patch(2, rows)))

    def pull():
        intensity = product(ordered[...], pick_t[...])

        def act(value, rows):
            misfit = value[0] * value[0] + value[1] * value[1] - intensity[rows]
            if live is not None:
                misfit = misfit * live
            return misfit * value[0], misfit * value[1]

        frequency(act)()

    def inward(value, rows):
        put(field, rows, conj_times(patch(2, rows), value))
        add(2, rows, conj_times(pair(passed, rows), value))

    def first(value, rows):
        add(0, rows, conj_times(pair(light, rows), value))

    return (
        wave, across, frequency(mix), down, space(second),
        across, pull, down, space(inward),
        across, frequency(revert), down, space(first),
    )


def slot_kernel(
    offsets, count, intensity, light, spread, table, table_t, pick, pick_t, ext, blank, acc,
    measured, field, upper, folded, passed, ordered, sems,
):
    number = count[0]
    steps = lax.div(number + 1, 2)

    def fetch(i, buf):
        return pltpu.make_async_copy(
            intensity.at[pl.ds(2 * i, 2)], measured.at[buf], sems.at[buf]
        )

    @pl.when(steps > 0)
    def _():
        fetch(0, 0).start()

    def one(i, carry):
        buf = lax.rem(i, 2)
        fetch(i, buf).wait()

        @pl.when(i + 1 < steps)
        def _():
            fetch(i + 1, 1 - buf).start()

        live = (2 * i + 1 < number).astype(jnp.float32)
        stages = [
            one_slot(
                k, live if k else None, offsets[0, 2 * i + k] + 1, offsets[1, 2 * i + k] + 1,
                light, spread, table, table_t, pick, pick_t, ext, acc, measured.at[buf, k],
                field.at[k], upper.at[k], folded.at[k], passed.at[k], ordered.at[k],
            )
            for k in range(2)
        ]
        for together in zip(*stages):
            for stage in together:
                stage()
        return carry

    lax.fori_loop(0, steps, one, 0)


def run_slots(offsets, count, intensity, light, spread, constants, ext, acc):
    smem = pl.BlockSpec(memory_space=pltpu.SMEM)
    vmem = pl.BlockSpec(memory_space=pltpu.VMEM)
    return pl.pallas_call(
        slot_kernel,
        out_shape=pltpu.VMEM(ext.shape, jnp.float32),
        in_specs=[smem, smem, pl.BlockSpec(memory_space=pltpu.HBM)] + [vmem] * 8,
        out_specs=vmem,
        scratch_shapes=[
            pltpu.VMEM((2, 2, EXTENT, EXTENT), jnp.bfloat16),
            pltpu.VMEM((2, 2, EXTENT, EXTENT), jnp.bfloat16),
            pltpu.VMEM((2, 2, EXTENT, EXTENT), jnp.bfloat16),
            pltpu.VMEM((2, 2, EXTENT, EXTENT), jnp.bfloat16),
            pltpu.VMEM((2, 2, EXTENT, EXTENT), jnp.float32),
            pltpu.VMEM((2, EXTENT, EXTENT), jnp.bfloat16),
            pltpu.SemaphoreType.DMA((2,)),
        ],
        input_output_aliases={10: 0},
        compiler_params=pltpu.CompilerParams(vmem_limit_bytes=16 * 2**20),
        cost_estimate=pl.CostEstimate(flops=12 * 26 * 2**25, bytes_accessed=2**24, transcendentals=0),
    )(offsets, count, intensity, light, spread, *constants, ext, acc)


def per_device(objects, illumination, propagator_phase, intensity, offsets, counts):
    constants = tables(EXTENT)
    ext, spread, acc = halo(objects, propagator_phase, *constants[2:])
    acc = run_slots(offsets.T, counts, intensity, illumination, spread, constants, ext, acc)
    return margins(acc, objects.shape[1])


def solution(mesh):
    placed = (
        P(None, "row", "col"),
        P(),
        P(),
        P(("row", "col"), None, None),
        P(("row", "col"), None),
        P(("row", "col")),
    )
    return jax.shard_map(
        per_device, mesh=mesh, in_specs=placed, out_specs=P(None, "row", "col"), check_vma=False
    )
```

```python
import math

import jax
import jax.numpy as jnp
import numpy as np
from jax import lax
from jax.experimental import pallas as pl
from jax.experimental.pallas import tpu as pltpu
from jax.sharding import PartitionSpec as P

EXTENT = 256
HALF = EXTENT // 2
MESH = pl.DeviceIdType.MESH


def tables(extent):
    half = extent // 2
    number = np.arange(extent, dtype=np.int32)
    turns = number[:, None] * number[None, :] % extent
    angle = turns.astype(np.float32) * np.float32(2.0 * math.pi / extent)
    scale = np.float32(1.0 / math.sqrt(extent))
    cosine = (np.cos(angle) * scale).astype(jnp.bfloat16)
    sine = (np.sin(angle) * scale).astype(jnp.bfloat16)
    folded = np.concatenate([cosine[:, : half + 1], sine[:, 1:half]], axis=1)
    order = np.concatenate([number[: half + 1], extent - number[1:half]])
    pick = np.eye(extent, dtype=np.float32)[order].astype(jnp.bfloat16)
    return tuple(jnp.asarray(np.ascontiguousarray(x)) for x in (folded, folded.T, pick, pick.T))


def product(a, b):
    return jnp.dot(a, b, preferred_element_type=jnp.float32)


def half(x):
    return x.astype(jnp.bfloat16)


SEAM = (7, 8)
RELAYS = ((3, 10), (5, 12))
PARTNERS = {7: (3, 5), 8: (10, 12), 3: (7, 10), 5: (7, 12), 10: (8, 3), 12: (8, 5)}


class Place:
    def __init__(self):
        r, c = lax.axis_index("row"), lax.axis_index("col")
        self.r, self.c = r, c
        self.has_above, self.has_below = r > 0, r < lax.axis_size("row") - 1
        self.has_left, self.has_right = c > 0, c < lax.axis_size("col") - 1
        self.above, self.below = (r - 1, c), (r + 1, c)
        self.left, self.right = (r, c - 1), (r, c + 1)
        self.sides = (
            (self.has_above, self.above),
            (self.has_below, self.below),
            (self.has_left, self.left),
            (self.has_right, self.right),
        )

    def greet(self):
        barrier = pltpu.get_barrier_semaphore()
        for there, device in self.sides:
            @pl.when(there)
            def _(device=device):
                pl.semaphore_signal(barrier, inc=1, device_id=device, device_id_type=MESH)

        for column, partners in PARTNERS.items():
            @pl.when(self.c == column)
            def _(partners=partners):
                for other in partners:
                    pl.semaphore_signal(barrier, inc=1, device_id=(self.r, other), device_id_type=MESH)

        count = sum(there.astype(jnp.int32) for there, _ in self.sides)
        count = count + 2 * sum((self.c == column).astype(jnp.int32) for column in PARTNERS)
        pl.semaphore_wait(barrier, count)


class Sends:
    def __init__(self, send, recv):
        self.send, self.recv, self.all = send, recv, {}

    def add(self, key, source, target, device, sent, received):
        k = len(self.all)
        copy = pltpu.make_async_remote_copy(
            src_ref=source, dst_ref=target, send_sem=self.send.at[k], recv_sem=self.recv.at[k],
            device_id=device, device_id_type=MESH,
        )
        self.all[key] = (copy, sent, received)

    def start(self, *keys):
        for key in keys:
            copy, sent, _ = self.all[key]
            pl.when(sent)(copy.start)

    def wait_recv(self, *keys):
        for key in keys:
            copy, _, received = self.all[key]
            pl.when(received)(copy.wait_recv)

    def relay(self, place, sources, targets, near, far):
        for g, pair in enumerate(RELAYS):
            planes = pl.ds(2 * g, 2)
            for side in range(2):
                device = tuple((place.r, column) for column in (pair[side], pair[1 - side], SEAM[side]))
                here = tuple(place.c == column for column in (pair[side], pair[1 - side], SEAM[side]))
                self.add(f"seam1{g}{side}", sources[side](planes), near, device[0], here[2], here[0])
                self.add(f"seam2{g}{side}", near, far, device[1], here[0], here[1])
                self.add(f"seam3{g}{side}", far, targets[side](planes), device[2], here[0], here[2])

    def start_seam(self, step):
        self.start(*(f"seam{step}{g}{side}" for g in range(2) for side in range(2)))

    def wait_seam(self, step):
        self.wait_recv(*(f"seam{step}{g}{side}" for g in range(2) for side in range(2)))

    def wait_sent(self, where, *keys):
        for key in keys:
            copy, sent, received = self.all[key]
            pl.when(both(sent, where))(copy.wait_send)
            self.all[key] = (copy, both(sent, jnp.logical_not(where)), received)

    def wait_seam_sent(self, place):
        relay = sum((place.c == column).astype(jnp.int32) for pair in RELAYS for column in pair) > 0
        self.wait_sent(relay, *(f"seam2{g}{side}" for g in range(2) for side in range(2)))

    def wait_send(self):
        for copy, sent, _ in self.all.values():
            pl.when(sent)(copy.wait_send)


def both(a, b):
    return jnp.logical_and(a, b)


def halo_kernel(
    objects, phase, pick, pick_t, ext, spread, acc, stage, angle, order, near_relay, far_relay,
    loads, send, recv
):
    tile = objects.shape[1]
    near, far, end = HALF, HALF + tile, 2 * HALF + tile
    own = slice(near, far)
    first, last = slice(0, near), slice(far, end)
    top, bottom = slice(near, 2 * near), slice(tile, far)
    place = Place()
    bands = ((tile - HALF, HALF), (0, HALF), (HALF, tile - 2 * HALF))
    loading = [
        pltpu.make_async_copy(objects.at[:, pl.ds(at, size)], stage.at[:, pl.ds(at, size)], loads.at[k])
        for k, (at, size) in enumerate(bands)
    ]
    parameters = [
        pltpu.make_async_copy(source, target, loads.at[3 + k])
        for k, (source, target) in enumerate(
            ((phase, angle), (pick, order.at[0]), (pick_t, order.at[1]))
        )
    ]
    for copy in loading + parameters:
        copy.start()
    place.greet()

    sends = Sends(send, recv)

    def route(key, source, target, device, sent, received):
        sends.add(key, ext.at[(slice(None),) + source], ext.at[(slice(None),) + target], device, sent, received)

    middle = slice(2 * near, tile)
    every, early, late = slice(None), slice(0, 2), slice(2, 4)
    for name, planes, cols in (
        ("l", every, top), ("r", every, bottom), ("m", early, middle), ("n", late, middle)
    ):
        for way, source, target, device, sent, received in (
            ("down", bottom, first, place.below, place.has_below, place.has_above),
            ("up", top, last, place.above, place.has_above, place.has_below),
        ):
            sends.add(way + name, ext.at[planes, source, cols], ext.at[planes, target, cols],
                      device, sent, received)
    for k, (at, size) in enumerate(bands):
        rows = slice(near + at, near + at + size)
        at_left, at_right = place.c != SEAM[0], place.c != SEAM[1]
        route(f"right{k}", (rows, bottom), (rows, first), place.right,
              both(place.has_right, at_left), both(place.has_left, at_right))
        route(f"left{k}", (rows, top), (rows, last), place.left,
              both(place.has_left, at_right), both(place.has_right, at_left))
    sends.relay(
        place,
        (lambda p: ext.at[p, own, bottom], lambda p: ext.at[p, own, top]),
        (lambda p: ext.at[p, own, last], lambda p: ext.at[p, own, first]),
        near_relay, far_relay,
    )
    for name, rows, there in (("t", first, place.has_above), ("b", last, place.has_below)):
        route("right" + name, (rows, bottom), (rows, first), place.right,
              both(place.has_right, there), both(place.has_left, there))
        route("left" + name, (rows, top), (rows, last), place.left,
              both(place.has_left, there), both(place.has_right, there))

    def cast(k):
        loading[k].wait()
        at, size = bands[k]
        for plane in range(4):
            ext[plane, near + at:near + at + size, near:far] = stage[plane, at:at + size].astype(jnp.bfloat16)

    cast(0)
    sends.start("downl", "downr", "right0", "left0")
    cast(1)
    sends.start("upl", "upr", "right1", "left1")
    cast(2)
    sends.start("right2", "left2")
    sends.start_seam(1)
    sends.start("downm", "upm")

    def blank(there, rows, cols):
        @pl.when(jnp.logical_not(there))
        def _():
            part = ext.at[:, rows, cols]
            part[...] = jnp.zeros(part.shape, jnp.bfloat16)

    blank(place.has_above, first, own)
    blank(place.has_below, last, own)
    blank(place.has_left, own, first)
    blank(place.has_right, own, last)
    for rows, there in ((first, place.has_above), (last, place.has_below)):
        blank(both(there, place.has_left), rows, first)
        blank(both(there, place.has_right), rows, last)
    for copy in parameters:
        copy.wait()
    rest, ordered = angle[...], 0.0
    for _ in range(3):
        part = half(rest)
        rest = rest - part.astype(jnp.float32)
        ordered = ordered + product(half(product(order[0], part)), order[1])
    spread[0] = jnp.cos(ordered)
    spread[1] = jnp.sin(ordered)
    for plane in range(4):
        acc[plane] = jnp.zeros(acc.shape[1:], jnp.float32)

    sends.wait_seam(1)
    sends.start_seam(2)
    sends.wait_recv("downl", "downr")
    sends.start("leftt", "rightt")
    sends.wait_recv("upl", "upr")
    sends.start("leftb", "rightb")
    sends.wait_seam_sent(place)
    sends.wait_sent(place.c == SEAM[0], "rightt", "rightb")
    sends.wait_sent(place.c == SEAM[1], "leftt", "leftb")
    sends.start("downn", "upn")
    sends.wait_seam(2)
    sends.start_seam(3)
    sends.wait_recv(*(f"{side}{k}" for side in ("right", "left") for k in range(3)))
    sends.wait_seam(3)
    sends.wait_recv("downn", "upn", "downm", "upm", "leftt", "rightt", "leftb", "rightb")
    sends.wait_send()


def halo(objects, phase, pick, pick_t):
    tile = objects.shape[1]
    size = tile + 2 * HALF
    relay = pltpu.VMEM((2, tile, HALF), jnp.bfloat16)
    vmem = pl.BlockSpec(memory_space=pltpu.VMEM)
    return pl.pallas_call(
        halo_kernel,
        out_shape=(
            pltpu.VMEM((4, size, size), jnp.bfloat16),
            pltpu.VMEM((2, EXTENT, EXTENT), jnp.float32),
            pltpu.VMEM((4, size, size), jnp.float32),
        ),
        in_specs=[pl.BlockSpec(memory_space=pltpu.HBM)] * 4,
        out_specs=(vmem, vmem, vmem),
        scratch_shapes=[
            pltpu.VMEM(objects.shape, jnp.float32),
            pltpu.VMEM((EXTENT, EXTENT), jnp.float32),
            pltpu.VMEM((2, EXTENT, EXTENT), jnp.bfloat16),
            relay,
            relay,
            pltpu.SemaphoreType.DMA((6,)),
            pltpu.SemaphoreType.DMA((30,)),
            pltpu.SemaphoreType.DMA((30,)),
        ],
        compiler_params=pltpu.CompilerParams(
            collective_id=0, has_side_effects=True, vmem_limit_bytes=24 * 2**20
        ),
    )(*(pltpu.with_memory_space_constraint(x, pltpu.HBM) for x in (objects, phase, pick, pick_t)))


def margin_kernel(
    acc, out, row_send, row_recv, col_send, col_recv, corner_send, corner_recv,
    near_relay, far_relay, send, recv
):
    tile = out.shape[1]
    near, far, end = HALF, HALF + tile, 2 * HALF + tile
    own = slice(near, far)
    edges = (slice(0, near), slice(far, end))
    inner = slice(near, tile - near)
    outer = (slice(0, near), slice(tile - near, tile))
    place = Place()
    place.greet()
    rows = ((place.has_above, place.above), (place.has_below, place.below))
    cols = ((place.has_left, place.left), (place.has_right, place.right))

    sends = Sends(send, recv)
    for side, (there, device) in enumerate(cols):
        back = cols[1 - side][0]
        sends.add(f"corner{side}", corner_send.at[side], corner_recv.at[1 - side], device, there, back)
        sends.add(f"col{side}", col_send.at[side], col_recv.at[1 - side], device,
                  both(there, place.c != SEAM[1 - side]), both(back, place.c != SEAM[side]))
    sends.relay(
        place,
        (lambda p: col_send.at[1, p], lambda p: col_send.at[0, p]),
        (lambda p: col_recv.at[1, p], lambda p: col_recv.at[0, p]),
        near_relay, far_relay,
    )
    for side, (there, device) in enumerate(rows):
        back = rows[1 - side][0]
        for name, part in (("m", inner), ("l", outer[0]), ("r", outer[1])):
            sends.add(
                f"row{side}{name}", row_send.at[side, :, :, part], row_recv.at[1 - side, :, :, part],
                device, there, back,
            )

    for c in range(2):
        for r in range(2):
            corner_send[c, r] = acc[:, edges[r], edges[c]].astype(jnp.bfloat16)
        sends.start(f"corner{c}")
    for c in range(2):
        for plane in range(4):
            col_send[c, plane] = acc[plane, own, edges[c]].astype(jnp.bfloat16)
    sends.start_seam(1)
    for r in range(2):
        row_send[r, :, :, inner] = acc[:, edges[r], 2 * near:tile].astype(jnp.bfloat16)
        sends.start(f"row{r}m")
    sends.start("col0", "col1")

    for side in range(2):
        @pl.when(jnp.logical_not(cols[side][0]))
        def _(side=side):
            corner_recv[side] = jnp.zeros(corner_recv.shape[1:], jnp.bfloat16)
            col_recv[side] = jnp.zeros(col_recv.shape[1:], jnp.bfloat16)

        @pl.when(jnp.logical_not(rows[side][0]))
        def _(side=side):
            row_recv[side] = jnp.zeros(row_recv.shape[1:], jnp.bfloat16)

    sends.wait_recv("corner0", "corner1")
    for c, name in enumerate("lr"):
        if c == 1:
            sends.wait_seam(1)
            sends.start_seam(2)
            sends.wait_seam_sent(place)
        for r in range(2):
            at = slice(near + outer[c].start, near + outer[c].stop)
            total = acc[:, edges[r], at] + corner_recv[c, r].astype(jnp.float32)
            row_send[r, :, :, outer[c]] = total.astype(jnp.bfloat16)
            sends.start(f"row{r}{name}")

    for plane in range(4):
        out[plane] = acc[plane, own, own]
    sends.wait_seam(2)
    sends.start_seam(3)
    sends.wait_recv("col0", "col1")
    sends.wait_seam(3)
    for c in range(2):
        for plane in range(4):
            out[plane, :, outer[c]] += col_recv[c, plane].astype(jnp.float32)
    sends.wait_recv("row0m", "row1m", "row0l", "row1l", "row0r", "row1r")
    for r in range(2):
        for plane in range(4):
            out[plane, outer[r], :] += row_recv[r, plane].astype(jnp.float32)
    sends.wait_send()


def margins(acc, tile):
    vmem = pl.BlockSpec(memory_space=pltpu.VMEM)
    row = pltpu.VMEM((2, 4, HALF, tile), jnp.bfloat16)
    col = pltpu.VMEM((2, 4, tile, HALF), jnp.bfloat16)
    relay = pltpu.VMEM((2, tile, HALF), jnp.bfloat16)
    corner = pltpu.VMEM((2, 2, 4, HALF, HALF), jnp.bfloat16)
    return pl.pallas_call(
        margin_kernel,
        out_shape=pltpu.VMEM((4, tile, tile), jnp.float32),
        in_specs=[vmem],
        out_specs=vmem,
        scratch_shapes=[
            row, row, col, col, corner, corner, relay, relay,
            pltpu.SemaphoreType.DMA((22,)),
            pltpu.SemaphoreType.DMA((22,)),
        ],
        compiler_params=pltpu.CompilerParams(
            collective_id=1, has_side_effects=True, vmem_limit_bytes=32 * 2**20
        ),
    )(acc)


def output_fold(a, b, first):
    (ca, sa), (cb, sb) = a, b
    if first is None:
        return (ca + sb, cb - sa), (ca - sb, cb + sa)
    sa0, sb0 = jnp.where(first, 0.0, sa), jnp.where(first, 0.0, sb)
    low, high = jnp.where(first, sa, ca), jnp.where(first, sb, cb)
    return (ca + sb0, cb - sa0), (low - sb0, high + sa0)


def input_fold(top, bottom, first):
    (tr, ti), (br, bi) = top, bottom
    if first is None:
        return (tr + br, bi - ti), (ti + bi, tr - br)
    br0, bi0 = jnp.where(first, 0.0, br), jnp.where(first, 0.0, bi)
    return (tr + br0, jnp.where(first, br, bi - ti)), (ti + bi0, jnp.where(first, bi, tr - br))


def times(a, b):
    return a[0] * b[0] - a[1] * b[1], a[0] * b[1] + a[1] * b[0]


def conj_times(a, b):
    return a[0] * b[0] + a[1] * b[1], a[0] * b[1] - a[1] * b[0]


ROWS = 32
FULL = tuple(slice(r, r + ROWS) for r in range(0, EXTENT, ROWS))
UPPER = FULL[: len(FULL) // 2]
LEFT, RIGHT = slice(0, HALF), slice(HALF, EXTENT)


def one_slot(k, live, row, col, light, spread, table, table_t, pick, pick_t, ext, acc, measured,
             field, upper, folded, passed, ordered):
    cols = pl.ds(pl.multiple_of(col * HALF, HALF), EXTENT)
    lane = lax.broadcasted_iota(jnp.int32, (ROWS, HALF), 1) == 0
    top_row = lax.broadcasted_iota(jnp.int32, (ROWS, EXTENT), 0) == 0

    def place(rows):
        return pl.ds(pl.multiple_of(row * HALF + rows.start, ROWS), ROWS)

    def patch(plane, rows):
        at = place(rows)
        return tuple(ext[plane + i, at, cols].astype(jnp.float32) for i in range(2))

    def pair(ref, rows):
        return ref[0, rows, :], ref[1, rows, :]

    def put(ref, rows, value, columns=slice(None)):
        ref[0, rows, columns] = half(value[0])
        ref[1, rows, columns] = half(value[1])

    def add(plane, rows, value):
        at = place(rows)
        for i in range(2):
            acc[plane + i, at, cols] += value[i]

    def wave():
        for rows in FULL:
            put(field, rows, times(pair(light, rows), patch(0, rows)))
        ordered[...] = half(product(pick[...], measured[...]))

    def across():
        a, b = product(field[0], table[...]), product(field[1], table[...])
        for rows in FULL:
            low, high = output_fold(
                (a[rows, LEFT], a[rows, RIGHT]), (b[rows, LEFT], b[rows, RIGHT]), lane
            )
            put(upper, rows, low, LEFT)
            put(upper, rows, high, RIGHT)

    def frequency(act):
        def run():
            a, b = product(table_t[...], upper[0]), product(table_t[...], upper[1])
            for rows in UPPER:
                lower = slice(rows.start + HALF, rows.stop + HALF)
                first = top_row if rows.start == 0 else None
                low, high = output_fold((a[rows], a[lower]), (b[rows], b[lower]), first)
                x, y = input_fold(act(low, rows), act(high, lower), first)
                folded[0, rows, :], folded[0, lower, :] = half(x[0]), half(x[1])
                folded[1, rows, :], folded[1, lower, :] = half(y[0]), half(y[1])
        return run

    def down():
        a, b = product(table[...], folded[0]), product(table[...], folded[1])
        for rows in FULL:
            x, y = input_fold(
                (a[rows, LEFT], b[rows, LEFT]), (a[rows, RIGHT], b[rows, RIGHT]), lane
            )
            upper[0, rows, LEFT], upper[0, rows, RIGHT] = half(x[0]), half(x[1])
            upper[1, rows, LEFT], upper[1, rows, RIGHT] = half(y[0]), half(y[1])

    def space(act):
        def run():
            a, b = product(upper[0], table_t[...]), product(upper[1], table_t[...])
            for rows in FULL:
                act((a[rows], b[rows]), rows)
        return run

    def mix(value, rows):
        return times(pair(spread, rows), value)

    def revert(value, rows):
        return conj_times(pair(spread, rows), value)

    def second(value, rows):
        passed[0, rows, :], passed[1, rows, :] = value
        put(field, rows, times(value, patch(2, rows)))

    def pull():
        intensity = product(ordered[...], pick_t[...])

        def act(value, rows):
            misfit = value[0] * value[0] + value[1] * value[1] - intensity[rows]
            if live is not None:
                misfit = misfit * live
            return misfit * value[0], misfit * value[1]

        frequency(act)()

    def inward(value, rows):
        put(field, rows, conj_times(patch(2, rows), value))
        add(2, rows, conj_times(pair(passed, rows), value))

    def first(value, rows):
        add(0, rows, conj_times(pair(light, rows), value))

    return (
        wave, across, frequency(mix), down, space(second),
        across, pull, down, space(inward),
        across, frequency(revert), down, space(first),
    )


def slot_kernel(
    offsets, count, intensity, light, spread, table, table_t, pick, pick_t, ext, blank, acc,
    measured, field, upper, folded, passed, ordered, sems,
):
    number = count[0]
    steps = lax.div(number + 1, 2)

    def fetch(i, buf):
        return pltpu.make_async_copy(
            intensity.at[pl.ds(2 * i, 2)], measured.at[buf], sems.at[buf]
        )

    @pl.when(steps > 0)
    def _():
        fetch(0, 0).start()

    def one(i, carry):
        buf = lax.rem(i, 2)
        fetch(i, buf).wait()

        @pl.when(i + 1 < steps)
        def _():
            fetch(i + 1, 1 - buf).start()

        live = (2 * i + 1 < number).astype(jnp.float32)
        stages = [
            one_slot(
                k, live if k else None, offsets[0, 2 * i + k] + 1, offsets[1, 2 * i + k] + 1,
                light, spread, table, table_t, pick, pick_t, ext, acc, measured.at[buf, k],
                field.at[k], upper.at[k], folded.at[k], passed.at[k], ordered.at[k],
            )
            for k in range(2)
        ]
        for together in zip(*stages):
            for stage in together:
                stage()
        return carry

    lax.fori_loop(0, steps, one, 0)


def run_slots(offsets, count, intensity, light, spread, constants, ext, acc):
    smem = pl.BlockSpec(memory_space=pltpu.SMEM)
    vmem = pl.BlockSpec(memory_space=pltpu.VMEM)
    return pl.pallas_call(
        slot_kernel,
        out_shape=pltpu.VMEM(ext.shape, jnp.float32),
        in_specs=[smem, smem, pl.BlockSpec(memory_space=pltpu.HBM)] + [vmem] * 8,
        out_specs=vmem,
        scratch_shapes=[
            pltpu.VMEM((2, 2, EXTENT, EXTENT), jnp.bfloat16),
            pltpu.VMEM((2, 2, EXTENT, EXTENT), jnp.bfloat16),
            pltpu.VMEM((2, 2, EXTENT, EXTENT), jnp.bfloat16),
            pltpu.VMEM((2, 2, EXTENT, EXTENT), jnp.bfloat16),
            pltpu.VMEM((2, 2, EXTENT, EXTENT), jnp.float32),
            pltpu.VMEM((2, EXTENT, EXTENT), jnp.bfloat16),
            pltpu.SemaphoreType.DMA((2,)),
        ],
        input_output_aliases={10: 0},
        compiler_params=pltpu.CompilerParams(vmem_limit_bytes=16 * 2**20),
        cost_estimate=pl.CostEstimate(flops=12 * 26 * 2**25, bytes_accessed=2**24, transcendentals=0),
    )(offsets, count, intensity, light, spread, *constants, ext, acc)


def per_device(objects, illumination, propagator_phase, intensity, offsets, counts):
    constants = tables(EXTENT)
    ext, spread, acc = halo(objects, propagator_phase, *constants[2:])
    acc = run_slots(offsets.T, counts, intensity, illumination, spread, constants, ext, acc)
    return margins(acc, objects.shape[1])


def solution(mesh):
    placed = (
        P(None, "row", "col"),
        P(),
        P(),
        P(("row", "col"), None, None),
        P(("row", "col"), None),
        P(("row", "col")),
    )
    return jax.shard_map(
        per_device, mesh=mesh, in_specs=placed, out_specs=P(None, "row", "col"), check_vma=False
    )
```

```python
import math

import jax
import jax.numpy as jnp
import numpy as np
from jax import lax
from jax.experimental import pallas as pl
from jax.experimental.pallas import tpu as pltpu
from jax.sharding import PartitionSpec as P

EXTENT = 256
HALF = EXTENT // 2
MESH = pl.DeviceIdType.MESH


def tables(extent):
    half = extent // 2
    number = np.arange(extent, dtype=np.int32)
    turns = number[:, None] * number[None, :] % extent
    angle = turns.astype(np.float32) * np.float32(2.0 * math.pi / extent)
    scale = np.float32(1.0 / math.sqrt(extent))
    cosine = (np.cos(angle) * scale).astype(jnp.bfloat16)
    sine = (np.sin(angle) * scale).astype(jnp.bfloat16)
    folded = np.concatenate([cosine[:, : half + 1], sine[:, 1:half]], axis=1)
    order = np.concatenate([number[: half + 1], extent - number[1:half]])
    pick = np.eye(extent, dtype=np.float32)[order].astype(jnp.bfloat16)
    return tuple(jnp.asarray(np.ascontiguousarray(x)) for x in (folded, folded.T, pick, pick.T))


def product(a, b):
    return jnp.dot(a, b, preferred_element_type=jnp.float32)


def half(x):
    return x.astype(jnp.bfloat16)


SEAM = (7, 8)
RELAYS = ((3, 10), (5, 12))
PARTNERS = {7: (3, 5), 8: (10, 12), 3: (7, 10), 5: (7, 12), 10: (8, 3), 12: (8, 5)}


class Place:
    def __init__(self):
        r, c = lax.axis_index("row"), lax.axis_index("col")
        self.r, self.c = r, c
        self.has_above, self.has_below = r > 0, r < lax.axis_size("row") - 1
        self.has_left, self.has_right = c > 0, c < lax.axis_size("col") - 1
        self.above, self.below = (r - 1, c), (r + 1, c)
        self.left, self.right = (r, c - 1), (r, c + 1)
        self.sides = (
            (self.has_above, self.above),
            (self.has_below, self.below),
            (self.has_left, self.left),
            (self.has_right, self.right),
        )

    def greet(self):
        barrier = pltpu.get_barrier_semaphore()
        for there, device in self.sides:
            @pl.when(there)
            def _(device=device):
                pl.semaphore_signal(barrier, inc=1, device_id=device, device_id_type=MESH)

        for column, partners in PARTNERS.items():
            @pl.when(self.c == column)
            def _(partners=partners):
                for other in partners:
                    pl.semaphore_signal(barrier, inc=1, device_id=(self.r, other), device_id_type=MESH)

        count = sum(there.astype(jnp.int32) for there, _ in self.sides)
        count = count + 2 * sum((self.c == column).astype(jnp.int32) for column in PARTNERS)
        pl.semaphore_wait(barrier, count)


class Sends:
    def __init__(self, send, recv):
        self.send, self.recv, self.all = send, recv, {}

    def add(self, key, source, target, device, sent, received):
        k = len(self.all)
        copy = pltpu.make_async_remote_copy(
            src_ref=source, dst_ref=target, send_sem=self.send.at[k], recv_sem=self.recv.at[k],
            device_id=device, device_id_type=MESH,
        )
        self.all[key] = (copy, sent, received)

    def start(self, *keys):
        for key in keys:
            copy, sent, _ = self.all[key]
            pl.when(sent)(copy.start)

    def wait_recv(self, *keys):
        for key in keys:
            copy, _, received = self.all[key]
            pl.when(received)(copy.wait_recv)

    def relay(self, place, sources, targets, near, far):
        rest = pl.ds(2, 2)
        for side in range(2):
            self.add(f"seam{side}", sources[side](rest), targets[1 - side](rest),
                     (place.r, SEAM[1 - side]), place.c == SEAM[side], place.c == SEAM[1 - side])
        for g, pair in enumerate(RELAYS):
            planes = pl.ds(g, 1)
            for side in range(2):
                device = tuple((place.r, column) for column in (pair[side], pair[1 - side], SEAM[side]))
                here = tuple(place.c == column for column in (pair[side], pair[1 - side], SEAM[side]))
                self.add(f"seam1{g}{side}", sources[side](planes), near, device[0], here[2], here[0])
                self.add(f"seam2{g}{side}", near, far, device[1], here[0], here[1])
                self.add(f"seam3{g}{side}", far, targets[side](planes), device[2], here[0], here[2])

    def start_seam(self, step):
        self.start(*(f"seam{step}{g}{side}" for g in range(2) for side in range(2)))
        if step == 1:
            self.start("seam0", "seam1")

    def wait_seam(self, step):
        self.wait_recv(*(f"seam{step}{g}{side}" for g in range(2) for side in range(2)))
        if step == 3:
            self.wait_recv("seam0", "seam1")

    def wait_send(self):
        for copy, sent, _ in self.all.values():
            pl.when(sent)(copy.wait_send)


def both(a, b):
    return jnp.logical_and(a, b)


def halo_kernel(
    objects, phase, pick, pick_t, ext, spread, acc, stage, angle, order, near_relay, far_relay,
    loads, send, recv
):
    tile = objects.shape[1]
    near, far, end = HALF, HALF + tile, 2 * HALF + tile
    own = slice(near, far)
    first, last = slice(0, near), slice(far, end)
    top, bottom = slice(near, 2 * near), slice(tile, far)
    place = Place()
    bands = ((tile - HALF, HALF), (0, HALF), (HALF, tile - 2 * HALF))
    loading = [
        pltpu.make_async_copy(objects.at[:, pl.ds(at, size)], stage.at[:, pl.ds(at, size)], loads.at[k])
        for k, (at, size) in enumerate(bands)
    ]
    parameters = [
        pltpu.make_async_copy(source, target, loads.at[3 + k])
        for k, (source, target) in enumerate(
            ((phase, angle), (pick, order.at[0]), (pick_t, order.at[1]))
        )
    ]
    for copy in loading + parameters:
        copy.start()
    place.greet()

    sends = Sends(send, recv)

    def route(key, source, target, device, sent, received):
        sends.add(key, ext.at[(slice(None),) + source], ext.at[(slice(None),) + target], device, sent, received)

    middle = slice(2 * near, tile)
    every, early, late = slice(None), slice(0, 2), slice(2, 4)
    for name, planes, cols in (
        ("l", every, top), ("r", every, bottom), ("m", early, middle), ("n", late, middle)
    ):
        for way, source, target, device, sent, received in (
            ("down", bottom, first, place.below, place.has_below, place.has_above),
            ("up", top, last, place.above, place.has_above, place.has_below),
        ):
            sends.add(way + name, ext.at[planes, source, cols], ext.at[planes, target, cols],
                      device, sent, received)
    for k, (at, size) in enumerate(bands):
        rows = slice(near + at, near + at + size)
        at_left, at_right = place.c != SEAM[0], place.c != SEAM[1]
        route(f"right{k}", (rows, bottom), (rows, first), place.right,
              both(place.has_right, at_left), both(place.has_left, at_right))
        route(f"left{k}", (rows, top), (rows, last), place.left,
              both(place.has_left, at_right), both(place.has_right, at_left))
    sends.relay(
        place,
        (lambda p: ext.at[p, own, bottom], lambda p: ext.at[p, own, top]),
        (lambda p: ext.at[p, own, last], lambda p: ext.at[p, own, first]),
        near_relay, far_relay,
    )
    for name, rows, there in (("t", first, place.has_above), ("b", last, place.has_below)):
        route("right" + name, (rows, bottom), (rows, first), place.right,
              both(place.has_right, there), both(place.has_left, there))
        route("left" + name, (rows, top), (rows, last), place.left,
              both(place.has_left, there), both(place.has_right, there))

    def cast(k):
        loading[k].wait()
        at, size = bands[k]
        for plane in range(4):
            ext[plane, near + at:near + at + size, near:far] = stage[plane, at:at + size].astype(jnp.bfloat16)

    cast(0)
    sends.start("downl", "downr", "right0", "left0")
    cast(1)
    sends.start("upl", "upr", "right1", "left1")
    cast(2)
    sends.start("right2", "left2")
    sends.start_seam(1)
    sends.start("downm", "upm")

    def blank(there, rows, cols):
        @pl.when(jnp.logical_not(there))
        def _():
            part = ext.at[:, rows, cols]
            part[...] = jnp.zeros(part.shape, jnp.bfloat16)

    blank(place.has_above, first, own)
    blank(place.has_below, last, own)
    blank(place.has_left, own, first)
    blank(place.has_right, own, last)
    for rows, there in ((first, place.has_above), (last, place.has_below)):
        blank(both(there, place.has_left), rows, first)
        blank(both(there, place.has_right), rows, last)
    for copy in parameters:
        copy.wait()
    rest, ordered = angle[...], 0.0
    for _ in range(3):
        part = half(rest)
        rest = rest - part.astype(jnp.float32)
        ordered = ordered + product(half(product(order[0], part)), order[1])
    spread[0] = jnp.cos(ordered)
    spread[1] = jnp.sin(ordered)
    for plane in range(4):
        acc[plane] = jnp.zeros(acc.shape[1:], jnp.float32)

    sends.wait_seam(1)
    sends.start_seam(2)
    sends.wait_recv("downl", "downr")
    sends.start("leftt", "rightt")
    sends.wait_recv("upl", "upr")
    sends.start("leftb", "rightb")
    sends.start("downn", "upn")
    sends.wait_seam(2)
    sends.start_seam(3)
    sends.wait_recv(*(f"{side}{k}" for side in ("right", "left") for k in range(3)))
    sends.wait_seam(3)
    sends.wait_recv("downn", "upn", "downm", "upm", "leftt", "rightt", "leftb", "rightb")
    sends.wait_send()


def halo(objects, phase, pick, pick_t):
    tile = objects.shape[1]
    size = tile + 2 * HALF
    relay = pltpu.VMEM((1, tile, HALF), jnp.bfloat16)
    vmem = pl.BlockSpec(memory_space=pltpu.VMEM)
    return pl.pallas_call(
        halo_kernel,
        out_shape=(
            pltpu.VMEM((4, size, size), jnp.bfloat16),
            pltpu.VMEM((2, EXTENT, EXTENT), jnp.float32),
            pltpu.VMEM((4, size, size), jnp.float32),
        ),
        in_specs=[pl.BlockSpec(memory_space=pltpu.HBM)] * 4,
        out_specs=(vmem, vmem, vmem),
        scratch_shapes=[
            pltpu.VMEM(objects.shape, jnp.float32),
            pltpu.VMEM((EXTENT, EXTENT), jnp.float32),
            pltpu.VMEM((2, EXTENT, EXTENT), jnp.bfloat16),
            relay,
            relay,
            pltpu.SemaphoreType.DMA((6,)),
            pltpu.SemaphoreType.DMA((32,)),
            pltpu.SemaphoreType.DMA((32,)),
        ],
        compiler_params=pltpu.CompilerParams(
            collective_id=0, has_side_effects=True, vmem_limit_bytes=24 * 2**20
        ),
    )(*(pltpu.with_memory_space_constraint(x, pltpu.HBM) for x in (objects, phase, pick, pick_t)))


def margin_kernel(
    acc, out, row_send, row_recv, col_send, col_recv, corner_send, corner_recv,
    near_relay, far_relay, send, recv
):
    tile = out.shape[1]
    near, far, end = HALF, HALF + tile, 2 * HALF + tile
    own = slice(near, far)
    edges = (slice(0, near), slice(far, end))
    inner = slice(near, tile - near)
    outer = (slice(0, near), slice(tile - near, tile))
    place = Place()
    place.greet()
    rows = ((place.has_above, place.above), (place.has_below, place.below))
    cols = ((place.has_left, place.left), (place.has_right, place.right))

    sends = Sends(send, recv)
    for side, (there, device) in enumerate(cols):
        back = cols[1 - side][0]
        sends.add(f"corner{side}", corner_send.at[side], corner_recv.at[1 - side], device, there, back)
        sends.add(f"col{side}", col_send.at[side], col_recv.at[1 - side], device,
                  both(there, place.c != SEAM[1 - side]), both(back, place.c != SEAM[side]))
    sends.relay(
        place,
        (lambda p: col_send.at[1, p], lambda p: col_send.at[0, p]),
        (lambda p: col_recv.at[1, p], lambda p: col_recv.at[0, p]),
        near_relay, far_relay,
    )
    for side, (there, device) in enumerate(rows):
        back = rows[1 - side][0]
        for name, part in (("m", inner), ("l", outer[0]), ("r", outer[1])):
            sends.add(
                f"row{side}{name}", row_send.at[side, :, :, part], row_recv.at[1 - side, :, :, part],
                device, there, back,
            )

    for c in range(2):
        for r in range(2):
            corner_send[c, r] = acc[:, edges[r], edges[c]].astype(jnp.bfloat16)
        sends.start(f"corner{c}")
    for c in range(2):
        for plane in range(4):
            col_send[c, plane] = acc[plane, own, edges[c]].astype(jnp.bfloat16)
    sends.start_seam(1)
    for r in range(2):
        row_send[r, :, :, inner] = acc[:, edges[r], 2 * near:tile].astype(jnp.bfloat16)
        sends.start(f"row{r}m")
    sends.start("col0", "col1")

    for side in range(2):
        @pl.when(jnp.logical_not(cols[side][0]))
        def _(side=side):
            corner_recv[side] = jnp.zeros(corner_recv.shape[1:], jnp.bfloat16)
            col_recv[side] = jnp.zeros(col_recv.shape[1:], jnp.bfloat16)

        @pl.when(jnp.logical_not(rows[side][0]))
        def _(side=side):
            row_recv[side] = jnp.zeros(row_recv.shape[1:], jnp.bfloat16)

    sends.wait_recv("corner0", "corner1")
    for c, name in enumerate("lr"):
        if c == 1:
            sends.wait_seam(1)
            sends.start_seam(2)
        for r in range(2):
            at = slice(near + outer[c].start, near + outer[c].stop)
            total = acc[:, edges[r], at] + corner_recv[c, r].astype(jnp.float32)
            row_send[r, :, :, outer[c]] = total.astype(jnp.bfloat16)
            sends.start(f"row{r}{name}")

    for plane in range(4):
        out[plane] = acc[plane, own, own]
    sends.wait_seam(2)
    sends.start_seam(3)
    sends.wait_recv("col0", "col1")
    sends.wait_seam(3)
    for c in range(2):
        for plane in range(4):
            out[plane, :, outer[c]] += col_recv[c, plane].astype(jnp.float32)
    sends.wait_recv("row0m", "row1m", "row0l", "row1l", "row0r", "row1r")
    for r in range(2):
        for plane in range(4):
            out[plane, outer[r], :] += row_recv[r, plane].astype(jnp.float32)
    sends.wait_send()


def margins(acc, tile):
    vmem = pl.BlockSpec(memory_space=pltpu.VMEM)
    row = pltpu.VMEM((2, 4, HALF, tile), jnp.bfloat16)
    col = pltpu.VMEM((2, 4, tile, HALF), jnp.bfloat16)
    relay = pltpu.VMEM((1, tile, HALF), jnp.bfloat16)
    corner = pltpu.VMEM((2, 2, 4, HALF, HALF), jnp.bfloat16)
    return pl.pallas_call(
        margin_kernel,
        out_shape=pltpu.VMEM((4, tile, tile), jnp.float32),
        in_specs=[vmem],
        out_specs=vmem,
        scratch_shapes=[
            row, row, col, col, corner, corner, relay, relay,
            pltpu.SemaphoreType.DMA((24,)),
            pltpu.SemaphoreType.DMA((24,)),
        ],
        compiler_params=pltpu.CompilerParams(
            collective_id=1, has_side_effects=True, vmem_limit_bytes=32 * 2**20
        ),
    )(acc)


def output_fold(a, b, first):
    (ca, sa), (cb, sb) = a, b
    if first is None:
        return (ca + sb, cb - sa), (ca - sb, cb + sa)
    sa0, sb0 = jnp.where(first, 0.0, sa), jnp.where(first, 0.0, sb)
    low, high = jnp.where(first, sa, ca), jnp.where(first, sb, cb)
    return (ca + sb0, cb - sa0), (low - sb0, high + sa0)


def input_fold(top, bottom, first):
    (tr, ti), (br, bi) = top, bottom
    if first is None:
        return (tr + br, bi - ti), (ti + bi, tr - br)
    br0, bi0 = jnp.where(first, 0.0, br), jnp.where(first, 0.0, bi)
    return (tr + br0, jnp.where(first, br, bi - ti)), (ti + bi0, jnp.where(first, bi, tr - br))


def times(a, b):
    return a[0] * b[0] - a[1] * b[1], a[0] * b[1] + a[1] * b[0]


def conj_times(a, b):
    return a[0] * b[0] + a[1] * b[1], a[0] * b[1] - a[1] * b[0]


ROWS = 32
FULL = tuple(slice(r, r + ROWS) for r in range(0, EXTENT, ROWS))
UPPER = FULL[: len(FULL) // 2]
LEFT, RIGHT = slice(0, HALF), slice(HALF, EXTENT)


def one_slot(k, live, row, col, light, spread, table, table_t, pick, pick_t, ext, acc, measured,
             field, upper, folded, passed, ordered):
    cols = pl.ds(pl.multiple_of(col * HALF, HALF), EXTENT)
    lane = lax.broadcasted_iota(jnp.int32, (ROWS, HALF), 1) == 0
    top_row = lax.broadcasted_iota(jnp.int32, (ROWS, EXTENT), 0) == 0

    def place(rows):
        return pl.ds(pl.multiple_of(row * HALF + rows.start, ROWS), ROWS)

    def patch(plane, rows):
        at = place(rows)
        return tuple(ext[plane + i, at, cols].astype(jnp.float32) for i in range(2))

    def pair(ref, rows):
        return ref[0, rows, :], ref[1, rows, :]

    def put(ref, rows, value, columns=slice(None)):
        ref[0, rows, columns] = half(value[0])
        ref[1, rows, columns] = half(value[1])

    def add(plane, rows, value):
        at = place(rows)
        for i in range(2):
            acc[plane + i, at, cols] += value[i]

    def wave():
        for rows in FULL:
            put(field, rows, times(pair(light, rows), patch(0, rows)))
        ordered[...] = half(product(pick[...], measured[...]))

    def across():
        a, b = product(field[0], table[...]), product(field[1], table[...])
        for rows in FULL:
            low, high = output_fold(
                (a[rows, LEFT], a[rows, RIGHT]), (b[rows, LEFT], b[rows, RIGHT]), lane
            )
            put(upper, rows, low, LEFT)
            put(upper, rows, high, RIGHT)

    def frequency(act):
        def run():
            a, b = product(table_t[...], upper[0]), product(table_t[...], upper[1])
            for rows in UPPER:
                lower = slice(rows.start + HALF, rows.stop + HALF)
                first = top_row if rows.start == 0 else None
                low, high = output_fold((a[rows], a[lower]), (b[rows], b[lower]), first)
                x, y = input_fold(act(low, rows), act(high, lower), first)
                folded[0, rows, :], folded[0, lower, :] = half(x[0]), half(x[1])
                folded[1, rows, :], folded[1, lower, :] = half(y[0]), half(y[1])
        return run

    def down():
        a, b = product(table[...], folded[0]), product(table[...], folded[1])
        for rows in FULL:
            x, y = input_fold(
                (a[rows, LEFT], b[rows, LEFT]), (a[rows, RIGHT], b[rows, RIGHT]), lane
            )
            upper[0, rows, LEFT], upper[0, rows, RIGHT] = half(x[0]), half(x[1])
            upper[1, rows, LEFT], upper[1, rows, RIGHT] = half(y[0]), half(y[1])

    def space(act):
        def run():
            a, b = product(upper[0], table_t[...]), product(upper[1], table_t[...])
            for rows in FULL:
                act((a[rows], b[rows]), rows)
        return run

    def mix(value, rows):
        return times(pair(spread, rows), value)

    def revert(value, rows):
        return conj_times(pair(spread, rows), value)

    def second(value, rows):
        passed[0, rows, :], passed[1, rows, :] = value
        put(field, rows, times(value, patch(2, rows)))

    def pull():
        intensity = product(ordered[...], pick_t[...])

        def act(value, rows):
            misfit = value[0] * value[0] + value[1] * value[1] - intensity[rows]
            if live is not None:
                misfit = misfit * live
            return misfit * value[0], misfit * value[1]

        frequency(act)()

    def inward(value, rows):
        put(field, rows, conj_times(patch(2, rows), value))
        add(2, rows, conj_times(pair(passed, rows), value))

    def first(value, rows):
        add(0, rows, conj_times(pair(light, rows), value))

    return (
        wave, across, frequency(mix), down, space(second),
        across, pull, down, space(inward),
        across, frequency(revert), down, space(first),
    )


def slot_kernel(
    offsets, count, intensity, light, spread, table, table_t, pick, pick_t, ext, blank, acc,
    measured, field, upper, folded, passed, ordered, sems,
):
    number = count[0]
    steps = lax.div(number + 1, 2)

    def fetch(i, buf):
        return pltpu.make_async_copy(
            intensity.at[pl.ds(2 * i, 2)], measured.at[buf], sems.at[buf]
        )

    @pl.when(steps > 0)
    def _():
        fetch(0, 0).start()

    def one(i, carry):
        buf = lax.rem(i, 2)
        fetch(i, buf).wait()

        @pl.when(i + 1 < steps)
        def _():
            fetch(i + 1, 1 - buf).start()

        live = (2 * i + 1 < number).astype(jnp.float32)
        stages = [
            one_slot(
                k, live if k else None, offsets[0, 2 * i + k] + 1, offsets[1, 2 * i + k] + 1,
                light, spread, table, table_t, pick, pick_t, ext, acc, measured.at[buf, k],
                field.at[k], upper.at[k], folded.at[k], passed.at[k], ordered.at[k],
            )
            for k in range(2)
        ]
        for together in zip(*stages):
            for stage in together:
                stage()
        return carry

    lax.fori_loop(0, steps, one, 0)


def run_slots(offsets, count, intensity, light, spread, constants, ext, acc):
    smem = pl.BlockSpec(memory_space=pltpu.SMEM)
    vmem = pl.BlockSpec(memory_space=pltpu.VMEM)
    return pl.pallas_call(
        slot_kernel,
        out_shape=pltpu.VMEM(ext.shape, jnp.float32),
        in_specs=[smem, smem, pl.BlockSpec(memory_space=pltpu.HBM)] + [vmem] * 8,
        out_specs=vmem,
        scratch_shapes=[
            pltpu.VMEM((2, 2, EXTENT, EXTENT), jnp.bfloat16),
            pltpu.VMEM((2, 2, EXTENT, EXTENT), jnp.bfloat16),
            pltpu.VMEM((2, 2, EXTENT, EXTENT), jnp.bfloat16),
            pltpu.VMEM((2, 2, EXTENT, EXTENT), jnp.bfloat16),
            pltpu.VMEM((2, 2, EXTENT, EXTENT), jnp.float32),
            pltpu.VMEM((2, EXTENT, EXTENT), jnp.bfloat16),
            pltpu.SemaphoreType.DMA((2,)),
        ],
        input_output_aliases={10: 0},
        compiler_params=pltpu.CompilerParams(vmem_limit_bytes=16 * 2**20),
        cost_estimate=pl.CostEstimate(flops=12 * 26 * 2**25, bytes_accessed=2**24, transcendentals=0),
    )(offsets, count, intensity, light, spread, *constants, ext, acc)


def per_device(objects, illumination, propagator_phase, intensity, offsets, counts):
    constants = tables(EXTENT)
    ext, spread, acc = halo(objects, propagator_phase, *constants[2:])
    acc = run_slots(offsets.T, counts, intensity, illumination, spread, constants, ext, acc)
    return margins(acc, objects.shape[1])


def solution(mesh):
    placed = (
        P(None, "row", "col"),
        P(),
        P(),
        P(("row", "col"), None, None),
        P(("row", "col"), None),
        P(("row", "col")),
    )
    return jax.shard_map(
        per_device, mesh=mesh, in_specs=placed, out_specs=P(None, "row", "col"), check_vma=False
    )
```
